32 devices in a mesh: seq: 8 (over y, x, core), batch: 4 (over z).
Axes of the slice: x: 2, y: 2, z: 4, core: 2. Of those that a mesh axis runs over, the one named last changes fastest.
Arguments:
- tokens: bfloat16 [4, 1024, 1024], P('batch', 'seq'), may hold values from -6 to 6
- out_grad: bfloat16 [4, 1024, 1024], P('batch', 'seq'), may hold values from -6 to 6
- group_id: int32 [4], P('batch'), may hold values from 0 to 7
- group_weight: float32 [8], replicated, may hold values from 0.25 to 4
- gain_attn: float32 [1024], P(('seq', 'batch')), may hold values from 0.5 to 1.5
- w_query: float32 [1024, 1024], P(('seq', 'batch')), may hold values from -0.1875 to 0.1875
- w_qrope: float32 [1024, 1024], P(('seq', 'batch')), may hold values from -0.1875 to 0.1875
- w_latent: float32 [1024, 512], P(('seq', 'batch')), may hold values from -0.1875 to 0.1875
- w_krope: float32 [1024, 64], P(('seq', 'batch')), may hold values from -0.1875 to 0.1875
- w_ukey: float32 [1024, 256], P(('seq', 'batch')), may hold values from -0.75 to 0.75
- w_uval: float32 [1024, 256], P(('seq', 'batch')), may hold values from -0.375 to 0.375
- w_out: float32 [1024, 1024], P(('seq', 'batch')), may hold values from -1.5 to 1.5
- gain_ffn: float32 [1024], P(('seq', 'batch')), may hold values from 0.5 to 1.5
- w_gate: float32 [1024, 2816], P(('seq', 'batch')), may hold values from -0.1875 to 0.1875
- w_up: float32 [1024, 2816], P(('seq', 'batch')), may hold values from -0.1875 to 0.1875
- w_down: float32 [2816, 1024], P(('seq', 'batch')), may hold values from -0.109375 to 0.109375
Outputs:
- block_out: bfloat16 [4, 1024, 1024], P('batch', 'seq')
- tokens_grad: float32 [4, 1024, 1024], P('batch', 'seq')
- gain_attn_grad: float32 [1024], P(('seq', 'batch'))
- w_query_grad: float32 [1024, 1024], P(('seq', 'batch'))
- w_qrope_grad: float32 [1024, 1024], P(('seq', 'batch'))
- w_latent_grad: float32 [1024, 512], P(('seq', 'batch'))
- w_krope_grad: float32 [1024, 64], P(('seq', 'batch'))
- w_ukey_grad: float32 [1024, 256], P(('seq', 'batch'))
- w_uval_grad: float32 [1024, 256], P(('seq', 'batch'))
- w_out_grad: float32 [1024, 1024], P(('seq', 'batch'))
- gain_ffn_grad: float32 [1024], P(('seq', 'batch'))
- w_gate_grad: float32 [1024, 2816], P(('seq', 'batch'))
- w_up_grad: float32 [1024, 2816], P(('seq', 'batch'))
- w_down_grad: float32 [2816, 1024], P(('seq', 'batch'))
The draws below stay inside these ranges and needn't reach their ends.
Inputs may be any that keep to these rules, and one draw needn't show every extreme that they name: `group_id`: each sequence's domain group, an index into group_weight.
All inputs are finite; a program needn't handle non-finite values.
Results may differ from the reference program's by a relative error of at most 0.02.
Values may be sent and summed in bfloat16 or wider, within the bound.
A program may use at most 256 MiB of HBM per device.

```python
import math
import jax
import jax.numpy as jnp
import numpy as np
from jax import lax

D = 1024
FF = 2816
H = 16
HD = 64
GROUPS = 2
LAT = 256
ROPE = 64
NDOM = 8
SEQS = 4
LENGTH = 1024


def touch_ends(drawn, key, low, top_value):
    spot = [jax.random.randint(jax.random.fold_in(key, axis), (), 0, length) for axis, length in enumerate(drawn.shape)]
    longest = drawn.shape.index(max(drawn.shape))
    beside = spot[:longest] + [(spot[longest] + 1) % drawn.shape[longest]] + spot[longest + 1:]
    return drawn.at[tuple(spot)].set(low).at[tuple(beside)].set(top_value)


def spiked(array, key, source, target, blocks, factor):
    def block_of(dim):
        return (jnp.arange(array.shape[dim]) // (array.shape[dim] // blocks)).reshape((-1,) + (1,) * (array.ndim - 1 - dim))

    one_side = jax.random.permutation(key, blocks)[block_of(target)]
    far = (block_of(target) + blocks // 2) % blocks
    return jnp.where((block_of(source) == one_side) | (block_of(source) == far), factor * array, array)


def steps_of(own_key, shape, split, low, largest):
    def one(axis_at, shards_of):
        steps = jax.random.uniform(jax.random.fold_in(jax.random.fold_in(own_key, 6), axis_at), (shards_of,), jnp.float32, low / len(split), largest / len(split))
        return jnp.repeat(jnp.exp(steps), shape[axis_at] // shards_of).reshape((-1,) + (1,) * (len(shape) - axis_at - 1))

    gain = one(*split[0])
    for cut in split[1:]:
        gain = gain * one(*cut)
    return gain


def cumulative_ranks(number_of, skew):
    weights = [(1 << 20) // math.isqrt(standing ** skew) + 1 for standing in range(1, number_of + 1)]
    scale = 1 + sum(weights) // (1 << 30)
    return np.cumsum(np.array([max(1, weight // scale) for weight in weights]))


def ranked(key, shape, number_of, slope):
    table = cumulative_ranks(number_of, slope)
    ticket = jax.random.randint(jax.random.fold_in(key, 1), shape, 0, int(table[number_of - 1]))
    rank = jnp.searchsorted(jnp.asarray(table, jnp.int32), ticket, side="right")
    return jax.random.permutation(jax.random.fold_in(key, 2), number_of)[rank].astype(jnp.int32)


def gaussian(own_key, dims, deviation, bound, split=(), held_as=jnp.bfloat16):
    drawn = deviation * jax.random.normal(own_key, dims, jnp.float32)
    if split:
        drawn = drawn * steps_of(own_key, dims, split, -0.22, 0.18)
    return jnp.clip(drawn, -bound, bound).astype(held_as)


def noise_with(stream_key, dims, width, bound, cuts, heavy, dtype=jnp.bfloat16):
    array = width * jax.random.normal(stream_key, dims, jnp.float32)
    if cuts:
        array = array * steps_of(stream_key, dims, cuts, -0.22, 0.18)
    return jnp.clip(spiked(array, jax.random.fold_in(stream_key, 3), *heavy), -bound, bound).astype(dtype)


def setup_inputs(seed: int = 0) -> dict:
    keys = jax.random.split(jax.random.key(seed), 17)
    return {
        "tokens": noise_with(keys[0], (SEQS, LENGTH, D), 1.0, 6.0, ((0, 4), (1, 8)), (1, 2, 8, 2.0)),
        "out_grad": gaussian(keys[1], (SEQS, LENGTH, D), 1.0, 6.0, ((0, 4), (1, 8))),
        "group_id": touch_ends(ranked(keys[2], (SEQS,), NDOM, 2), jax.random.fold_in(keys[2], 3), 0, NDOM - 1).astype(jnp.int32),
        "group_weight": jnp.clip(jnp.exp(jax.random.uniform(keys[3], (NDOM,), jnp.float32, math.log(0.25), math.log(4.0))), 0.25, 4.0),
        "gain_attn": jnp.clip(1.0 + 0.1 * jax.random.normal(keys[4], (D,), jnp.float32), 0.5, 1.5),
        "w_query": gaussian(keys[5], (D, H * HD), D ** -0.5, 0.1875, ((0, 32),), jnp.float32),
        "w_qrope": gaussian(keys[6], (D, H * ROPE), D ** -0.5, 0.1875, ((0, 32),), jnp.float32),
        "w_latent": gaussian(keys[7], (D, GROUPS * LAT), D ** -0.5, 0.1875, ((0, 32),), jnp.float32),
        "w_krope": gaussian(keys[8], (D, ROPE), D ** -0.5, 0.1875, ((0, 32),), jnp.float32),
        "w_ukey": gaussian(keys[9], (H * HD, LAT), HD ** -0.5, 0.75, ((0, 32),), jnp.float32),
        "w_uval": gaussian(keys[10], (H * HD, LAT), LAT ** -0.5, 0.375, ((0, 32),), jnp.float32),
        "w_out": gaussian(keys[11], (H * HD, D), (H * HD // 64) ** -0.5, 1.5, ((0, 32),), jnp.float32),
        "gain_ffn": jnp.clip(1.0 + 0.1 * jax.random.normal(keys[12], (D,), jnp.float32), 0.5, 1.5),
        "w_gate": gaussian(keys[13], (D, FF), D ** -0.5, 0.1875, ((0, 32),), jnp.float32),
        "w_up": gaussian(keys[14], (D, FF), D ** -0.5, 0.1875, ((0, 32),), jnp.float32),
        "w_down": gaussian(keys[15], (FF, D), FF ** -0.5, 0.109375, ((0, 32),), jnp.float32),
    }


EPSILON = 1e-05
ROTARY_BASE = 10000.0
NEG_FILL = -1e+30

@jax.custom_vjp
def low(v):
    return lax.optimization_barrier(v.astype(jnp.bfloat16)).astype(jnp.float32)

@jax.custom_vjp
def low_back(v):
    return v

def low_keep(v):
    return (low(v), None)

def low_pass(kept, grad):
    return (grad,)

def back_keep(v):
    return (v, None)

def back_low(kept, grad):
    return (low(grad),)
low.defvjp(low_keep, low_pass)
low_back.defvjp(back_keep, back_low)

def highest(left_side, right_side):
    return jnp.dot(left_side, right_side, precision=lax.Precision.HIGHEST)

def rms_norm(values, norm_gain):
    return values * lax.rsqrt(lax.optimization_barrier(jnp.mean(values * values, -1, keepdims=True)) + EPSILON) * norm_gain

def rotate(values, position):
    half_width = values.shape[-1] // 2
    frequency = ROTARY_BASE ** (-jnp.arange(half_width).astype(jnp.float32) * 2.0 / values.shape[-1])
    angles = position[:, None] * frequency[None, :]
    cosine = jnp.cos(angles)[:, None, :]
    sine_part = jnp.sin(angles)[:, None, :]
    first_half = values[..., :half_width]
    second_half = values[..., half_width:]
    return jnp.concatenate([first_half * cosine - second_half * sine_part, first_half * sine_part + second_half * cosine], -1)

def layer(inputs, position, params):
    gain_a, query_w, qrope_w, latent_w, krope_w, ukey_w, uval_w, out_w, gain_f, gate_w, up_w, down_w = [low(master) for master in params]
    length = inputs.shape[0]
    per_group = H // GROUPS
    scaling = (HD + ROPE) ** (-0.5)
    precise = lax.Precision.HIGHEST
    normed = low(rms_norm(inputs, gain_a))
    queries = low(low_back(highest(normed, query_w))).reshape(length, H, HD)
    query_rope = low(rotate(low_back(highest(normed, qrope_w)).reshape(length, H, ROPE), position))
    latent = low(low_back(highest(normed, latent_w))).reshape(length, GROUPS, LAT)
    key_rope = low(rotate(low_back(highest(normed, krope_w)).reshape(length, 1, ROPE), position))[:, 0]
    query_latent = low(low_back(jnp.einsum('lhe,hef->lhf', queries, ukey_w.reshape(H, HD, LAT), precision=precise)))
    query_latent = query_latent.reshape(length, GROUPS, per_group, LAT)
    query_rope = query_rope.reshape(length, GROUPS, per_group, ROPE)
    block_rows = math.gcd(length, 512)
    block_count = length // block_rows
    positions = jnp.arange(length).astype(jnp.int32)

    def attend(payload):
        query_block, rope_block, query_pos = payload
        scores = jnp.einsum('qgpf,kgf->gpqk', query_block, latent, precision=precise)
        scores = (scores + jnp.einsum('qgpr,kr->gpqk', rope_block, key_rope, precision=precise)) * scaling
        scores = low_back(scores)
        scores = jnp.where(positions[None, :] <= query_pos[:, None], scores, NEG_FILL)
        probability = jax.nn.softmax(scores, axis=-1)
        return jnp.einsum('gpqk,kgf->qgpf', low(probability), latent, precision=precise)
    out_latent = lax.map(jax.checkpoint(attend), (query_latent.reshape(block_count, block_rows, GROUPS, per_group, LAT), query_rope.reshape(block_count, block_rows, GROUPS, per_group, ROPE), positions.reshape(block_count, block_rows)))
    out_latent = low(low_back(out_latent.reshape(length, H, LAT)))
    head_out = low(low_back(jnp.einsum('lhf,hef->lhe', out_latent, uval_w.reshape(H, HD, LAT), precision=precise))).reshape(length, H * HD)
    residual = inputs + low_back(highest(head_out, out_w))
    normed_f = low(rms_norm(residual, gain_f))
    gate_pre = low_back(highest(normed_f, gate_w))
    up_pre = low_back(highest(normed_f, up_w))
    hidden = low(jax.nn.silu(gate_pre) * up_pre)
    return residual + low_back(highest(hidden, down_w))

def reference(tokens, out_grad, group_id, group_weight, gain_attn, w_query, w_qrope, w_latent, w_krope, w_ukey, w_uval, w_out, gain_ffn, w_gate, w_up, w_down):
    params = (gain_attn, w_query, w_qrope, w_latent, w_krope, w_ukey, w_uval, w_out, gain_ffn, w_gate, w_up, w_down)
    position = jnp.arange(LENGTH).astype(jnp.int32).astype(jnp.float32)

    def one_sequence(running, payload):
        inputs, cotangent, group_index = payload
        weight = jnp.sum(jnp.where(jnp.arange(NDOM).astype(jnp.int32) == group_index, group_weight, 0.0))

        def forward(input_vals, param_set):
            return layer(input_vals, position, param_set)
        result, pullback = jax.vjp(forward, inputs.astype(jnp.float32), params)
        input_grad, param_grads = pullback(weight * cotangent.astype(jnp.float32))
        return (jax.tree.map(jnp.add, running, param_grads), (result.astype(jnp.bfloat16), input_grad))
    zeros_init = tuple((jnp.zeros_like(master) for master in params))
    gradients, (outputs, input_grads) = lax.scan(one_sequence, zeros_init, (tokens, out_grad, group_id))
    return (outputs, input_grads, gradients[0], gradients[1], gradients[2], gradients[3], gradients[4], gradients[5], gradients[6], gradients[7], gradients[8], gradients[9], gradients[10], gradients[11])
```

```python
import jax
import jax.numpy as jnp
from jax import lax
from jax.sharding import PartitionSpec as P

FF = 2816
H = 16
HD = 64
GROUPS = 2
LAT = 256
ROPE = 64
PER_GROUP = H // GROUPS

EPSILON = 1e-05
ROTARY_BASE = 10000.0
NEG_FILL = -1e30
BF = jnp.bfloat16
F32 = jnp.float32


def mm(a, b):
    return jnp.dot(a, b, preferred_element_type=F32)


def mm_tn(a, b):
    return lax.dot_general(a, b, (((0,), (0,)), ((), ())), preferred_element_type=F32)


def mm_nt(a, b):
    return lax.dot_general(a, b, (((1,), (1,)), ((), ())), preferred_element_type=F32)


def rms(v, g):
    inv = lax.rsqrt(jnp.mean(v * v, -1, keepdims=True) + EPSILON)
    return inv, v * inv * g


def rms_grad(v, inv, g, dn):
    scaled = dn * g
    back = inv * scaled - v * (inv * inv * inv) * jnp.mean(scaled * v, -1, keepdims=True)
    return back, jnp.sum(dn * v * inv, 0)


def rotate(v, cosine, sine):
    half = v.shape[-1] // 2
    lo, hi = v[..., :half], v[..., half:]
    return jnp.concatenate([lo * cosine - hi * sine, lo * sine + hi * cosine], -1)


def seq_gather(v):
    return lax.all_gather(v, "seq", axis=0, tiled=True)


def seq_sum(v):
    return lax.psum_scatter(v.astype(BF), "seq", scatter_dimension=0, tiled=True).astype(F32)


def batch_gather(v):
    return lax.all_gather(v, "batch", axis=0, tiled=True)


def batch_sum(v):
    return lax.psum_scatter(v.astype(BF), "batch", scatter_dimension=0, tiled=True).astype(F32)


def local(
    tokens,
    out_grad,
    group_id,
    group_weight,
    gain_attn,
    w_query,
    w_qrope,
    w_latent,
    w_krope,
    w_ukey,
    w_uval,
    w_out,
    gain_ffn,
    w_gate,
    w_up,
    w_down,
):
    ns, nb = lax.axis_size("seq"), lax.axis_size("batch")
    seq_count, rows, width = tokens.shape
    shard = w_query.shape[0]
    length = rows * ns
    hl = H // ns
    fl = FF // ns
    qw, rw = hl * HD, hl * ROPE
    scaling = (HD + ROPE) ** (-0.5)

    def columns(w, blocks):
        return w.astype(BF).reshape(shard, blocks, -1).transpose(1, 0, 2)

    lat_cols = jnp.repeat(columns(w_latent, GROUPS), ns // GROUPS, axis=0)
    kr_cols = jnp.broadcast_to(w_krope.astype(BF)[None], (ns, shard, ROPE))
    send = jnp.concatenate(
        [columns(w_query, ns), columns(w_qrope, ns), lat_cols, kr_cols, columns(w_gate, ns), columns(w_up, ns)], -1
    )
    got = lax.all_to_all(send, "seq", 0, 0)
    wide = send.shape[-1]
    full = lax.all_gather(got, "batch", axis=1).reshape(width, wide)
    attn_w = qw + rw + LAT + ROPE
    wcat, wgu = full[:, :attn_w], full[:, attn_w:]
    ukey = batch_gather(w_ukey.astype(BF))
    uval = batch_gather(w_uval.astype(BF))
    wout = batch_gather(w_out.astype(BF))
    wdown = batch_gather(w_down.astype(BF))
    gains = lax.all_gather(
        jnp.stack([gain_attn, gain_ffn]).astype(BF), ("seq", "batch"), axis=1, tiled=True
    ).astype(F32)
    gain_a, gain_f = gains[0], gains[1]

    x = tokens.reshape(rows, width)
    domains = jnp.arange(group_weight.shape[0])
    seq_weight = jnp.sum(jnp.where(group_id[:, None] == domains[None, :], group_weight[None, :], 0.0), -1)
    gy = (out_grad.astype(F32) * seq_weight[:, None, None]).reshape(rows, width)
    dy_all = seq_gather(gy.astype(BF))
    x_all = seq_gather(x)
    x32 = x.astype(F32)

    position = jnp.arange(length).astype(F32)
    freq = ROTARY_BASE ** (-jnp.arange(ROPE // 2).astype(F32) * 2.0 / ROPE)
    angles = position[:, None] * freq
    cosine, sine = jnp.cos(angles), jnp.sin(angles)

    _, normed = rms(x_all.astype(F32), gain_a)
    a_all = normed.astype(BF)
    qkv = mm(a_all, wcat)
    q = qkv[:, :qw].astype(BF)
    qr = rotate(qkv[:, qw : qw + rw].reshape(length, hl, ROPE), cosine[:, None], sine[:, None]).astype(BF)
    c = qkv[:, qw + rw : qw + rw + LAT].astype(BF)
    kr = rotate(qkv[:, qw + rw + LAT :], cosine, sine).astype(BF)
    causal = jnp.arange(length)[None, :] <= jnp.arange(length)[:, None]

    keep = []
    outs = []
    for h in range(hl):
        uh = ukey[h * HD : (h + 1) * HD]
        vh = uval[h * HD : (h + 1) * HD]
        ql = mm(q[:, h * HD : (h + 1) * HD], uh).astype(BF)
        sc = (mm_nt(ql, c) + mm_nt(qr[:, h], kr)) * scaling
        sc = jnp.where(causal, sc, NEG_FILL)
        top = jnp.max(sc, -1, keepdims=True)
        e = jnp.exp(sc - top)
        total = jnp.sum(e, -1, keepdims=True)
        ol = mm(e.astype(BF), c) / total
        olb = ol.astype(BF)
        outs.append(mm_nt(olb, vh).astype(BF))
        keep.append((ql, ol, olb, top + jnp.log(total)))
    o = jnp.concatenate(outs, -1)
    hres = x32 + seq_sum(mm(o, wout))
    inv_f, normed_f = rms(hres, gain_f)
    b_all = seq_gather(normed_f.astype(BF))
    gu = mm(b_all, wgu)
    gate, up = gu[:, :fl], gu[:, fl:]
    sig = jax.nn.sigmoid(gate)
    act = gate * sig
    hid = (act * up).astype(BF)
    y = seq_sum(mm(hid, wdown))
    result = (hres + y).astype(BF).reshape(seq_count, rows, width)

    dhid = mm_nt(dy_all, wdown)
    dgate = (dhid * up * sig * (1.0 + gate * (1.0 - sig))).astype(BF)
    dup = (dhid * act).astype(BF)
    dgu = jnp.concatenate([dgate, dup], -1)
    db = seq_sum(mm_nt(dgu, wgu))
    g_down = batch_sum(mm_tn(hid, dy_all))
    g_gu = mm_tn(b_all, dgu)
    back_f, gg_f = rms_grad(hres, inv_f, gain_f, db)
    dres = gy + back_f
    dat_all = seq_gather(dres.astype(BF))
    g_out = mm_tn(o, dat_all)
    do = mm_nt(dat_all, wout).astype(BF)

    dqs, dqps, g_uk, g_uv = [], [], [], []
    dc = jnp.zeros((length, LAT), F32)
    dkr = jnp.zeros((length, ROPE), F32)
    for h in range(hl):
        ql, ol, olb, lse = keep[h]
        uh = ukey[h * HD : (h + 1) * HD]
        vh = uval[h * HD : (h + 1) * HD]
        doh = do[:, h * HD : (h + 1) * HD]
        g_uv.append(mm_tn(doh, olb))
        dol = mm(doh, vh).astype(BF)
        delta = jnp.sum(dol.astype(F32) * ol, -1, keepdims=True)
        sc = (mm_nt(ql, c) + mm_nt(qr[:, h], kr)) * scaling
        p = jnp.exp(jnp.where(causal, sc, NEG_FILL) - lse)
        ds = (p * (mm_nt(dol, c) - delta)).astype(BF)
        dql = (scaling * mm(ds, c)).astype(BF)
        dqps.append(rotate(scaling * mm(ds, kr), cosine, -sine).astype(BF))
        dkr = dkr + scaling * mm_tn(ds, qr[:, h])
        dc = dc + mm_tn(p.astype(BF), dol) + scaling * mm_tn(ds, ql)
        g_uk.append(mm_tn(q[:, h * HD : (h + 1) * HD], dql))
        dqs.append(mm_nt(dql, uh).astype(BF))
    dkp = rotate(dkr, cosine, -sine).astype(BF)
    gcat = jnp.concatenate(dqs + dqps + [dc.astype(BF), dkp], -1)
    da = seq_sum(mm_nt(gcat, wcat))
    g_cat = mm_tn(a_all, gcat)
    inv_a, _ = rms(x32, gain_a)
    back_a, gg_a = rms_grad(x32, inv_a, gain_a, da)
    input_grad = (dres + back_a).reshape(seq_count, rows, width)

    def wide_sum(g):
        cols = g.shape[-1]
        part = lax.psum_scatter(
            g.astype(BF).reshape(ns, nb, shard, cols), "batch", scatter_dimension=1, tiled=True
        ).reshape(ns, shard, cols)
        return lax.all_to_all(part, "seq", 0, 0)

    def spread(v):
        return v.transpose(1, 0, 2).reshape(shard, -1)

    r_gu = wide_sum(g_gu)
    r_cat = wide_sum(g_cat).astype(F32)
    p_query = spread(r_cat[:, :, :qw])
    p_qrope = spread(r_cat[:, :, qw : qw + rw])
    p_latent = spread(
        r_cat[:, :, qw + rw : qw + rw + LAT].reshape(GROUPS, ns // GROUPS, shard, LAT).sum(1)
    )
    p_krope = r_cat[:, :, qw + rw + LAT :].sum(0)
    p_gate = spread(r_gu[:, :, :fl]).astype(F32)
    p_up = spread(r_gu[:, :, fl:]).astype(F32)
    g_head = batch_sum(jnp.concatenate([jnp.concatenate(g_uk, 0), jnp.concatenate(g_uv, 0), g_out], -1))
    gg = lax.psum_scatter(jnp.stack([gg_a, gg_f]), ("seq", "batch"), scatter_dimension=1, tiled=True)
    return (
        result,
        input_grad,
        gg[0],
        p_query,
        p_qrope,
        p_latent,
        p_krope,
        g_head[:, :LAT],
        g_head[:, LAT : 2 * LAT],
        g_head[:, 2 * LAT :],
        gg[1],
        p_gate,
        p_up,
        g_down,
    )


def solution(mesh):
    token, row, flat = P("batch", "seq", None), P(("seq", "batch"), None), P(("seq", "batch"))
    return jax.shard_map(
        local,
        mesh=mesh,
        in_specs=(token, token, P("batch"), P(), flat, row, row, row, row, row, row, row, flat, row, row, row),
        out_specs=(token, token, flat, row, row, row, row, row, row, row, flat, row, row, row),
        check_vma=False,
    )
```

```python
import jax
import jax.numpy as jnp
from jax import lax
from jax.experimental import pallas as pl
from jax.experimental.pallas import tpu as pltpu
from jax.sharding import PartitionSpec as P

FF = 2816
H = 16
HD = 64
GROUPS = 2
LAT = 256
ROPE = 64
HALF = LAT // 2
PAD = 128

EPSILON = 1e-05
ROTARY_BASE = 10000.0
NEG_FILL = -1e30
BF = jnp.bfloat16
F32 = jnp.float32
MESH = pl.DeviceIdType.MESH
DMA = pltpu.SemaphoreType.DMA
VMEM = pl.BlockSpec(memory_space=pltpu.VMEM)


def mm(a, b):
    return jnp.dot(a, b, preferred_element_type=F32)


def mm_tn(a, b):
    return lax.dot_general(a, b, (((0,), (0,)), ((), ())), preferred_element_type=F32)


def mm_nt(a, b):
    return lax.dot_general(a, b, (((1,), (1,)), ((), ())), preferred_element_type=F32)


def rms(v, g):
    inv = lax.rsqrt(jnp.mean(v * v, -1, keepdims=True) + EPSILON)
    return inv, v * inv * g


def rms_grad(v, inv, g, dn):
    scaled = dn * g
    back = inv * scaled - v * (inv * inv * inv) * jnp.mean(scaled * v, -1, keepdims=True)
    return back, jnp.sum(dn * v * inv, 0, keepdims=True)


def rotate(v, cosine, sine):
    half = v.shape[-1] // 2
    lo, hi = v[..., :half], v[..., half:]
    return jnp.concatenate([lo * cosine - hi * sine, lo * sine + hi * cosine], -1)


def last(mask):
    return mask.bit_length() - 1


def aligned(start, size):
    return pl.ds(pl.multiple_of(start, size), size)


class Place:
    def __init__(self, ns, nb):
        self.ns, self.nb, self.nc = ns, nb, ns // 2
        self.dims = last(self.nc)
        self.me = lax.axis_index("seq")
        self.bat = lax.axis_index("batch")
        self.core = lax.rem(self.me, 2)
        self.chip = self.me // 2
        self.sib = self.chip * 2 + 1 - self.core

    def across(self, mask, core):
        spot = self.chip
        for j in range(self.dims):
            if mask >> j & 1:
                step = core * (1 << j) + (1 - core) * (1 << (self.dims - 1 - j))
                spot = spot + step - 2 * step * lax.rem(spot // step, 2)
        return spot * 2 + core

    def at(self, mask):
        return self.across(mask, self.core)

    def sib_at(self, mask):
        return self.across(mask, 1 - self.core)

    def seq(self, src, dst, send, recv, to):
        return pltpu.make_async_remote_copy(src, dst, send, recv, device_id={"seq": to}, device_id_type=MESH)

    def batch(self, src, dst, send, recv, to):
        return pltpu.make_async_remote_copy(src, dst, send, recv, device_id={"batch": to}, device_id_type=MESH)

    def barrier(self, all_seq, all_batch):
        sem = pltpu.get_barrier_semaphore()
        if all_seq:
            peers = [lax.rem(self.me + t, self.ns) for t in range(1, self.ns)]
        else:
            peers = [self.sib] + [self.at(1 << j) for j in range(self.dims)]
        for to in peers:
            pl.semaphore_signal(sem, 1, device_id={"seq": to}, device_id_type=MESH)
        count = len(peers)
        if all_batch:
            for t in range(1, self.nb):
                to = lax.rem(self.bat + t, self.nb)
                pl.semaphore_signal(sem, 1, device_id={"batch": to}, device_id_type=MESH)
            pl.semaphore_wait(sem, count + self.nb - 1)
            return

        @pl.when(self.bat > 0)
        def _():
            pl.semaphore_signal(sem, 1, device_id={"batch": self.bat - 1}, device_id_type=MESH)

        @pl.when(self.bat < self.nb - 1)
        def _():
            pl.semaphore_signal(sem, 1, device_id={"batch": self.bat + 1}, device_id_type=MESH)

        up = (self.bat > 0).astype(jnp.int32)
        down = (self.bat < self.nb - 1).astype(jnp.int32)
        pl.semaphore_wait(sem, count + up + down)


class Gather:
    def __init__(self, place, src, out, chunks, sems):
        self.place, self.src, self.out, self.chunks = place, src, out, chunks
        self.rows = src.shape[0]
        self.send, self.recv, self.sib_send, self.sib_recv = sems

    @staticmethod
    def sems(ns, chunks):
        nc = ns // 2
        hops, blocks = max(nc - 1, 1) * chunks, nc * chunks
        return [DMA((hops,)), DMA((hops,)), DMA((blocks,)), DMA((blocks,))]

    def slot(self, dev, ch):
        n = self.rows // self.chunks
        return self.out.at[pl.ds(pl.multiple_of(dev * self.rows + ch * n, n), n)]

    def block(self, mask, ch):
        n = self.rows // self.chunks
        if mask == 0:
            return self.src.at[pl.ds(ch * n, n)]
        return self.slot(self.place.at(mask), ch)

    def sends(self, mask, ch):
        place, copies = self.place, []
        for j in range(last(mask) + 1, place.dims):
            i = ((mask | 1 << j) - 1) * self.chunks + ch
            copies.append(
                place.seq(
                    self.block(mask, ch),
                    self.slot(place.at(mask), ch),
                    self.send.at[i],
                    self.recv.at[i],
                    place.at(1 << j),
                )
            )
        i = mask * self.chunks + ch
        copies.append(
            place.seq(
                self.block(mask, ch), self.slot(place.at(mask), ch), self.sib_send.at[i], self.sib_recv.at[i], place.sib
            )
        )
        return copies

    def start(self):
        for ch in range(self.chunks):
            for copy in self.sends(0, ch):
                copy.start()

    def relay(self, masks=None):
        place = self.place
        for mask in masks or range(1, place.nc):
            for ch in range(self.chunks):
                i = (mask - 1) * self.chunks + ch
                spot = self.slot(place.at(mask), ch)
                place.seq(spot, spot, self.send.at[i], self.recv.at[i], place.at(1 << last(mask))).wait_recv()
                for copy in self.sends(mask, ch):
                    copy.start()

    def finish(self):
        place = self.place
        for mask in range(place.nc):
            for ch in range(self.chunks):
                for copy in self.sends(mask, ch):
                    copy.wait_send()
                i = mask * self.chunks + ch
                spot = self.slot(place.sib_at(mask), ch)
                place.seq(spot, spot, self.sib_send.at[i], self.sib_recv.at[i], place.sib).wait_recv()


class Scatter:
    def __init__(self, place, part, bufs, sems):
        self.place, self.part = place, part
        self.acc, self.land, self.sib_land = bufs
        self.send, self.recv, self.sib_send, self.sib_recv = sems
        self.rows = part.shape[0] // place.ns

    @staticmethod
    def sems(ns):
        nc = ns // 2
        return [DMA((max(nc - 1, 1),)), DMA((max(nc - 1, 1),)), DMA((nc,)), DMA((nc,))]

    @staticmethod
    def bufs(ns, rows, width):
        return [pltpu.VMEM((ns // 2, rows, width), BF)] * 3

    def own(self, dev):
        return self.part.at[aligned(dev * self.rows, self.rows)]

    def sibling(self, mask):
        place = self.place
        return place.seq(
            self.own(place.sib_at(mask)),
            self.sib_land.at[mask],
            self.sib_send.at[mask],
            self.sib_recv.at[mask],
            place.sib,
        )

    def hop(self, mask):
        place = self.place
        return place.seq(
            self.acc.at[mask],
            self.land.at[mask],
            self.send.at[mask - 1],
            self.recv.at[mask - 1],
            place.at(1 << last(mask)),
        )

    def start(self):
        for mask in reversed(range(self.place.nc)):
            self.sibling(mask).start()

    def step(self, mask):
        place = self.place
        self.sibling(mask).wait_recv()
        value = self.own(place.at(mask))[...].astype(F32) + self.sib_land[mask].astype(F32)
        for j in reversed(range(last(mask) + 1, place.dims)):
            self.hop(mask | 1 << j).wait_recv()
            value = value + self.land[mask | 1 << j].astype(F32)
        if mask:
            self.acc[mask] = value.astype(BF)
            self.hop(mask).start()
        return value

    def total(self):
        for mask in reversed(range(1, self.place.nc)):
            self.step(mask)
        return self.step(0)

    def finish(self):
        for mask in range(self.place.nc):
            self.sibling(mask).wait_send()
            if mask:
                self.hop(mask).wait_send()


class Line:
    def __init__(self, place, slots, sems):
        self.place, self.slots = place, slots
        self.send, self.recv = sems

    @staticmethod
    def sems(nb, parts):
        return [DMA((2 * nb * parts,)), DMA((2 * nb * parts,))]

    def copy(self, up, d, i):
        place = self.place
        block = place.bat - d if up else place.bat + d
        to = place.bat + 1 if up else place.bat - 1
        ref = self.slots[i](block)
        at = (int(up) * place.nb + d) * len(self.slots) + i
        return place.batch(ref, ref, self.send.at[at], self.recv.at[at], to)

    def sends(self, up, d):
        bat, nb = self.place.bat, self.place.nb
        return (bat - d >= 0) & (bat + 1 < nb) if up else (bat + d < nb) & (bat >= 1)

    def start(self, d, parts):
        for up in (True, False):

            @pl.when(self.sends(up, d))
            def _(up=up):
                for i in parts:
                    self.copy(up, d, i).start()

    def came(self, up, d):
        return self.place.bat - d >= 0 if up else self.place.bat + d < self.place.nb

    def relay(self, d, parts, then=None):
        bat, nb = self.place.bat, self.place.nb
        for up in (True, False):

            @pl.when(self.came(up, d))
            def _(up=up):
                for i in parts:
                    block = bat - d if up else bat + d
                    ref = self.slots[i](block)
                    at = (int(up) * nb + d - 1) * len(self.slots) + i
                    self.place.batch(ref, ref, self.send.at[at], self.recv.at[at], bat).wait_recv()
                    if d < nb - 1:

                        @pl.when(self.sends(up, d))
                        def _():
                            self.copy(up, d, i).start()

                    if then:
                        then(block, up, i)

    def finish(self, parts):
        for d in range(self.place.nb - 1):
            for up in (True, False):

                @pl.when(self.sends(up, d))
                def _(up=up, d=d):
                    for i in parts:
                        self.copy(up, d, i).wait_send()


class LineSum:
    def __init__(self, place, parts, bufs, sems):
        self.place, self.parts = place, parts
        self.bufs = [bufs[4 * i : 4 * i + 4] for i in range(len(parts))]
        self.send, self.recv = sems

    @staticmethod
    def sems(nb, parts):
        return [DMA((2 * nb * parts,)), DMA((2 * nb * parts,))]

    @staticmethod
    def scratch(nb, shapes):
        return [pltpu.VMEM((nb - 1,) + shape, BF) for shape in shapes for _ in range(4)]

    def copy(self, up, d, i, first):
        place = self.place
        land, acc = self.bufs[i][:2] if up else self.bufs[i][2:]
        to = place.bat + 1 if up else place.bat - 1
        dest = place.bat + d if up else place.bat - d
        src = self.parts[i](dest) if first else acc.at[d - 1]
        at = (int(up) * place.nb + d) * len(self.parts) + i
        return place.batch(src, land.at[d - 1], self.send.at[at], self.recv.at[at], to)

    def arrived(self, up, d, i):
        place = self.place
        land = self.bufs[i][0 if up else 2]
        at = (int(up) * place.nb + d + 1) * len(self.parts) + i
        place.batch(land.at[d], land.at[d], self.send.at[at], self.recv.at[at], place.bat).wait_recv()
        return land[d].astype(F32)

    def edge(self, up):
        return self.place.bat == 0 if up else self.place.bat == self.place.nb - 1

    def inside(self, up, d):
        return self.place.bat + d < self.place.nb if up else self.place.bat - d >= 0

    def start(self):
        for d in reversed(range(1, self.place.nb)):
            for up in (True, False):

                @pl.when(self.edge(up))
                def _(up=up, d=d):
                    for i in range(len(self.parts)):
                        self.copy(up, d, i, True).start()

    def stage(self, d):
        for up in (True, False):

            @pl.when(self.inside(up, d) & jnp.logical_not(self.edge(up)))
            def _(up=up):
                for i in range(len(self.parts)):
                    dest = self.place.bat + d if up else self.place.bat - d
                    acc = self.bufs[i][1 if up else 3]
                    acc[d - 1] = (self.parts[i](dest)[...].astype(F32) + self.arrived(up, d, i)).astype(BF)
                    self.copy(up, d, i, False).start()

    def total(self, outs):
        for i, out in enumerate(outs):
            out[...] = self.parts[i](self.place.bat)[...].astype(out.dtype)
            for up in (True, False):

                @pl.when(jnp.logical_not(self.edge(up)))
                def _(up=up):
                    out[...] = (out[...].astype(F32) + self.arrived(up, 0, i)).astype(out.dtype)

    def finish(self):
        for d in range(1, self.place.nb):
            for up in (True, False):

                @pl.when(self.inside(up, d) & self.edge(up))
                def _(up=up, d=d):
                    for i in range(len(self.parts)):
                        self.copy(up, d, i, True).wait_send()

                @pl.when(self.inside(up, d) & jnp.logical_not(self.edge(up)))
                def _(up=up, d=d):
                    for i in range(len(self.parts)):
                        self.copy(up, d, i, False).wait_send()


class Exchange:
    def __init__(self, place, pieces, slots, sems):
        self.place, self.pieces, self.slots = place, pieces, slots
        self.send, self.recv = sems

    @staticmethod
    def sems(ns, parts):
        return [DMA((ns * parts,)), DMA((ns * parts,))]

    def copy(self, t, i):
        place = self.place
        to = lax.rem(place.me + t, place.ns)
        at = t * len(self.pieces) + i
        src, dst = self.pieces[i](to), self.slots[i](place.me, to)
        if t == 0:
            return pltpu.make_async_copy(src, dst, self.recv.at[at])
        return place.seq(src, dst, self.send.at[at], self.recv.at[at], to)

    def start(self):
        for t in range(self.place.ns):
            for i in range(len(self.pieces)):
                self.copy(t, i).start()

    def arrive(self):
        place = self.place
        for t in range(place.ns):
            for i in range(len(self.pieces)):
                if t == 0:
                    self.copy(0, i).wait()
                    continue
                at = t * len(self.pieces) + i
                spot = self.slots[i](lax.rem(place.me + place.ns - t, place.ns), place.me)
                place.seq(spot, spot, self.send.at[at], self.recv.at[at], place.sib).wait_recv()

    def finish(self):
        for t in range(1, self.place.ns):
            for i in range(len(self.pieces)):
                self.copy(t, i).wait_send()


def take(refs, counts):
    out, at = [], 0
    for n in counts:
        out.append(refs[at : at + n])
        at += n
    return out


def comm_call(body, out_shape, scratch, cid, *args):
    return pl.pallas_call(
        body,
        out_shape=out_shape,
        in_specs=[VMEM] * len(args),
        out_specs=[VMEM] * len(out_shape),
        scratch_shapes=scratch,
        compiler_params=pltpu.CompilerParams(
            collective_id=cid, has_side_effects=True, vmem_limit_bytes=60 << 20
        ),
    )(*args)


def sds(shape, dtype):
    return jax.ShapeDtypeStruct(tuple(shape), dtype)


def fetch(ns, nb, x, dy, wide_a, wide_f, head_rows, chunks=4):
    rows, width = x.shape
    shard, aw = wide_a.shape[1:]
    qk = aw - HALF
    full = qk + LAT

    def body(x, dy, wa, wf, hr, x_all, dy_all, a_out, f_out, h_out, *rest):
        gx, gd, ea, ef, zl, local, sib = take(rest, (4, 4, 2, 2, 2, 1, 2))
        place = Place(ns, nb)
        local = local[0]
        mine = aligned(place.me * rows, rows)
        copies = [
            pltpu.make_async_copy(x, x_all.at[mine], local.at[0]),
            pltpu.make_async_copy(dy, dy_all.at[mine], local.at[1]),
            pltpu.make_async_copy(hr, h_out.at[place.bat], local.at[2]),
        ]
        for copy in copies:
            copy.start()
        place.barrier(True, False)

        def half(core):
            return pl.ds(pl.multiple_of(qk + HALF * core, HALF), HALF)

        cols = Exchange(
            place,
            [lambda to: wa.at[to, :, pl.ds(0, qk)], lambda to: wa.at[to, :, pl.ds(qk, HALF)]],
            [
                lambda frm, to: a_out.at[frm, place.bat, :, pl.ds(0, qk)],
                lambda frm, to: a_out.at[frm, place.bat, :, half(lax.rem(to, 2))],
            ],
            ea,
        )
        ffn = Exchange(place, [lambda to: wf.at[to]], [lambda frm, to: f_out.at[frm]], ef)
        along = Line(
            place,
            [
                lambda b: h_out.at[b],
                lambda b: a_out.at[:, b, :, pl.ds(0, qk)],
                lambda b: a_out.at[:, b, :, half(place.core)],
            ],
            zl,
        )

        def to_sibling(b, i):
            ref = a_out.at[:, b, :, half(place.core)]
            return place.seq(ref, ref, sib[0].at[i], sib[1].at[i], place.sib)

        xs, ds = Gather(place, x, x_all, chunks, gx), Gather(place, dy, dy_all, chunks, gd)
        cols.start()
        copies[2].wait()
        along.start(0, [0])
        xs.start()
        ffn.start()
        ds.start()
        cols.arrive()
        along.start(0, [1, 2])
        to_sibling(place.bat, 0).start()
        xs.relay()

        def then(b, up, d):
            to_sibling(b, d if up else nb - 1 + d).start()

        for d in range(1, nb):
            along.relay(d, [0])
        for d in range(1, nb):
            along.relay(d, [1])
            along.relay(d, [2], lambda b, up, i, d=d: then(b, up, d))
            if d == 1:
                ds.relay()
        ffn.arrive()
        xs.finish()
        ds.finish()
        cols.finish()
        ffn.finish()
        along.finish([0, 1, 2])

        def other(b, i):
            ref = a_out.at[:, b, :, half(1 - place.core)]
            place.seq(ref, ref, sib[0].at[i], sib[1].at[i], place.sib).wait_recv()

        to_sibling(place.bat, 0).wait_send()
        other(place.bat, 0)
        for d in range(1, nb):
            for up in (True, False):

                @pl.when(along.came(up, d))
                def _(up=up, d=d):
                    b = place.bat - d if up else place.bat + d
                    i = d if up else nb - 1 + d
                    to_sibling(b, i).wait_send()
                    other(b, i)

        copies[0].wait()
        copies[1].wait()

    scratch = (
        Gather.sems(ns, chunks)
        + Gather.sems(ns, chunks)
        + Exchange.sems(ns, 2)
        + Exchange.sems(ns, 1)
        + Line.sems(nb, 3)
        + [DMA((3,)), DMA((2 * nb,)), DMA((2 * nb,))]
    )
    return comm_call(
        body,
        [
            sds((ns * rows, width), BF),
            sds((ns * rows, width), BF),
            sds((ns, nb, shard, full), BF),
            sds(wide_f.shape, BF),
            sds((nb,) + head_rows.shape, BF),
        ],
        scratch,
        1,
        x,
        dy,
        wide_a,
        wide_f,
        head_rows,
    )


def turn_forward(ns, nb, part, x, gain, wide_f, down, chunks=4):
    rows, width = x.shape

    def body(part, x, gain, wf, dn, hres, b_all, f_out, d_out, own, *rest):
        bufs, rs, gs, zl, local = take(rest, (3, 4, 4, 2, 1))
        place = Place(ns, nb)
        local = local[0]
        copies = [
            pltpu.make_async_copy(wf, f_out.at[:, place.bat], local.at[0]),
            pltpu.make_async_copy(dn, d_out.at[place.bat], local.at[1]),
        ]
        for copy in copies:
            copy.start()
        place.barrier(False, False)
        sums = Scatter(place, part, bufs, rs)
        sums.start()
        along = Line(place, [lambda b: f_out.at[:, b], lambda b: d_out.at[b]], zl)
        for copy in copies:
            copy.wait()
        along.start(0, [0, 1])
        value = x[...].astype(F32) + sums.total()
        hres[...] = value
        own[...] = rms(value, gain[...])[1].astype(BF)
        spread = Gather(place, own, b_all, chunks, gs)
        spread.start()
        mine = pltpu.make_async_copy(own, b_all.at[aligned(place.me * rows, rows)], local.at[2])
        mine.start()
        along.relay(1, [0, 1])
        spread.relay()
        for d in range(2, nb):
            along.relay(d, [0, 1])
        spread.finish()
        sums.finish()
        along.finish([0, 1])
        mine.wait()

    scratch = (
        [pltpu.VMEM((rows, width), BF)]
        + Scatter.bufs(ns, rows, width)
        + Scatter.sems(ns)
        + Gather.sems(ns, chunks)
        + Line.sems(nb, 2)
        + [DMA((3,))]
    )
    return comm_call(
        body,
        [
            sds((rows, width), F32),
            sds((ns * rows, width), BF),
            sds((ns, nb) + wide_f.shape[1:], BF),
            sds((nb,) + down.shape, BF),
        ],
        scratch,
        2,
        part,
        x,
        gain,
        wide_f,
        down,
    )


def turn_back(ns, nb, part, gy, hres, gain, g_wide, g_down, chunks=4):
    rows, width = gy.shape

    def body(part, gy, hres, gain, gw, gd, dres, dat_all, gg, w_out, d_out, own, *rest):
        bufs, rs, gs, zb, zs, local = take(rest, (3, 4, 4, 8, 2, 1))
        place = Place(ns, nb)
        local = local[0]
        place.barrier(False, False)
        sums = Scatter(place, part, bufs, rs)
        sums.start()
        along = LineSum(place, [lambda b: gw.at[:, b], lambda b: gd.at[b]], zb, zs)
        along.start()
        db = sums.total()
        value = hres[...]
        inv = rms(value, gain[...])[0]
        back, gg[...] = rms_grad(value, inv, gain[...], db)
        value = gy[...] + back
        dres[...] = value
        own[...] = value.astype(BF)
        spread = Gather(place, own, dat_all, chunks, gs)
        spread.start()
        mine = pltpu.make_async_copy(own, dat_all.at[aligned(place.me * rows, rows)], local.at[0])
        mine.start()
        for d in reversed(range(1, nb - 1)):
            if d == nb - 3:
                spread.relay()
            along.stage(d)
        along.total([w_out, d_out])
        spread.finish()
        sums.finish()
        along.finish()
        mine.wait()

    scratch = (
        [pltpu.VMEM((rows, width), BF)]
        + Scatter.bufs(ns, rows, width)
        + Scatter.sems(ns)
        + Gather.sems(ns, chunks)
        + LineSum.scratch(nb, [(ns,) + g_wide.shape[2:], g_down.shape[1:]])
        + LineSum.sems(nb, 2)
        + [DMA((1,))]
    )
    return comm_call(
        body,
        [
            sds((rows, width), F32),
            sds((ns * rows, width), BF),
            sds((1, width), F32),
            sds((ns,) + g_wide.shape[2:], BF),
            sds(g_down.shape[1:], F32),
        ],
        scratch,
        3,
        part,
        gy,
        hres,
        gain,
        g_wide,
        g_down,
    )


def settle(ns, nb, part, part_y, x, hres, dres, gain, gg_f, g_cols, g_rows, g_wide):
    rows, width = x.shape

    def body(part, py, x, hres, dres, gain, ggf, gc, gr, gw, dx, y, gg, c_out, r_out, w_out, *rest):
        c_sum, g_own, g_seq, g_bat = rest[:4]
        ba, ra, by, ry, zb, zs, ec, ew, gs, gb = take(rest[4:], (3, 4, 3, 4, 8, 2, 2, 2, 2, 2))
        place = Place(ns, nb)
        place.barrier(True, True)
        sums, outs = Scatter(place, part, ba, ra), Scatter(place, py, by, ry)
        sums.start()
        along = LineSum(place, [lambda b: gc.at[:, b], lambda b: gr.at[b]], zb, zs)
        along.start()
        outs.start()
        wide = Exchange(place, [lambda to: gw.at[to]], [lambda frm, to: w_out.at[frm]], ew)
        da = sums.total()
        wide.start()
        value = x[...].astype(F32)
        inv = rms(value, gain[...])[0]
        back, gg_a = rms_grad(value, inv, gain[...], da)
        dx[...] = dres[...] + back
        g_own[pl.ds(0, 1)] = gg_a
        g_own[pl.ds(1, 1)] = ggf[...]
        gains = Exchange(place, [lambda to: g_own], [lambda frm, to: g_seq.at[frm]], gs)
        gains.start()
        stages = list(reversed(range(1, nb - 1)))
        for d in stages[:1]:
            along.stage(d)
        y[...] = (hres[...] + outs.total()).astype(BF)
        for d in stages[1:]:
            along.stage(d)
        gains.arrive()
        gains.finish()
        g_own[...] = jnp.sum(g_seq[...], 0)

        def gain_copy(t):
            to = lax.rem(place.bat + t, nb)
            return place.batch(g_own, g_bat.at[place.bat], gb[0].at[t], gb[1].at[t], to)

        for t in range(1, nb):
            gain_copy(t).start()
        along.total([c_sum, r_out])
        cols = Exchange(place, [lambda to: c_sum.at[to]], [lambda frm, to: c_out.at[frm]], ec)
        cols.start()
        g_bat[place.bat] = g_own[...]
        for t in range(1, nb):
            spot = g_bat.at[lax.rem(place.bat + nb - t, nb)]
            place.batch(spot, spot, gb[0].at[t], gb[1].at[t], place.bat).wait_recv()
        gg[...] = jnp.sum(g_bat[...], 0)
        wide.arrive()
        cols.arrive()
        for t in range(1, nb):
            gain_copy(t).wait_send()
        sums.finish()
        outs.finish()
        along.finish()
        wide.finish()
        cols.finish()

    block = (ns,) + g_cols.shape[2:]
    scratch = (
        [
            pltpu.VMEM(block, BF),
            pltpu.VMEM((2, width), F32),
            pltpu.VMEM((ns, 2, width), F32),
            pltpu.VMEM((nb, 2, width), F32),
        ]
        + Scatter.bufs(ns, rows, width)
        + Scatter.sems(ns)
        + Scatter.bufs(ns, rows, width)
        + Scatter.sems(ns)
        + LineSum.scratch(nb, [block, g_rows.shape[1:]])
        + LineSum.sems(nb, 2)
        + Exchange.sems(ns, 1)
        + Exchange.sems(ns, 1)
        + Exchange.sems(ns, 1)
        + [DMA((nb,)), DMA((nb,))]
    )
    return comm_call(
        body,
        [
            sds((rows, width), F32),
            sds((rows, width), BF),
            sds((2, width), F32),
            sds(block, BF),
            sds(g_rows.shape[1:], F32),
            sds(g_wide.shape, BF),
        ],
        scratch,
        4,
        part,
        part_y,
        x,
        hres,
        dres,
        gain,
        gg_f,
        g_cols,
        g_rows,
        g_wide,
    )


def local(
    tokens,
    out_grad,
    group_id,
    group_weight,
    gain_attn,
    w_query,
    w_qrope,
    w_latent,
    w_krope,
    w_ukey,
    w_uval,
    w_out,
    gain_ffn,
    w_gate,
    w_up,
    w_down,
):
    ns, nb = lax.axis_size("seq"), lax.axis_size("batch")
    me, bat = lax.axis_index("seq"), lax.axis_index("batch")
    seq_count, rows, width = tokens.shape
    shard = w_query.shape[0]
    length = rows * ns
    hl, fl = H // ns, FF // ns
    qw, rw = hl * HD, hl * ROPE
    scaling = (HD + ROPE) ** (-0.5)

    x = tokens.reshape(rows, width)
    domains = jnp.arange(group_weight.shape[0])
    seq_weight = jnp.sum(jnp.where(group_id[:, None] == domains[None, :], group_weight[None, :], 0.0), -1)
    gy = (out_grad.astype(F32) * seq_weight[:, None, None]).reshape(rows, width)

    def columns(w, blocks):
        return w.astype(BF).reshape(shard, blocks, -1).transpose(1, 0, 2)

    extra = jnp.concatenate(
        [
            w_krope.astype(BF),
            gain_attn.astype(BF)[:, None],
            gain_ffn.astype(BF)[:, None],
            jnp.zeros((shard, PAD - ROPE - 2), BF),
        ],
        1,
    )
    extra = jnp.broadcast_to(extra[None], (ns, shard, PAD))
    lat = columns(w_latent, GROUPS * 2).reshape(GROUPS, 1, 2, shard, HALF)
    lat = jnp.broadcast_to(lat, (GROUPS, ns // GROUPS // 2, 2, shard, HALF)).reshape(ns, shard, HALF)
    wide_a = jnp.concatenate([columns(w_query, ns), columns(w_qrope, ns), extra, lat], -1)
    wide_f = jnp.concatenate([columns(w_gate, ns), columns(w_up, ns)], -1)
    head_rows = jnp.concatenate([w_ukey, w_uval, w_out], 1).astype(BF)

    x_all, dy_all, acols, fcols, hrows = fetch(ns, nb, x, gy.astype(BF), wide_a, wide_f, head_rows)
    kr_at = qw + rw
    lat_at = kr_at + PAD
    full = lat_at + LAT
    wcat = acols.reshape(width, full)
    gains = wcat[:, kr_at + ROPE : kr_at + ROPE + 2].astype(F32).T
    gain_a, gain_f = gains[:1], gains[1:]
    hrows = hrows.reshape(nb * shard, -1)
    ukey, uval, wout = hrows[:, :LAT], hrows[:, LAT : 2 * LAT], hrows[:, 2 * LAT :]

    position = jnp.arange(length).astype(F32)
    freq = ROTARY_BASE ** (-jnp.arange(ROPE // 2).astype(F32) * 2.0 / ROPE)
    angles = position[:, None] * freq
    cosine, sine = jnp.cos(angles), jnp.sin(angles)

    a_all = rms(x_all.astype(F32), gain_a)[1].astype(BF)
    qkv = mm(a_all, wcat)
    q = qkv[:, :qw].astype(BF)
    qr = rotate(qkv[:, qw : qw + rw].reshape(length, hl, ROPE), cosine[:, None], sine[:, None]).astype(BF)
    c = qkv[:, lat_at:].astype(BF)
    kr = rotate(qkv[:, kr_at : kr_at + ROPE], cosine, sine).astype(BF)
    causal = jnp.arange(length)[None, :] <= jnp.arange(length)[:, None]

    keep = []
    outs = []
    for h in range(hl):
        uh = ukey[h * HD : (h + 1) * HD]
        vh = uval[h * HD : (h + 1) * HD]
        ql = mm(q[:, h * HD : (h + 1) * HD], uh).astype(BF)
        sc = (mm_nt(ql, c) + mm_nt(qr[:, h], kr)) * scaling
        sc = jnp.where(causal, sc, NEG_FILL)
        top = jnp.max(sc, -1, keepdims=True)
        e = jnp.exp(sc - top)
        total = jnp.sum(e, -1, keepdims=True)
        ol = mm(e.astype(BF), c) / total
        olb = ol.astype(BF)
        outs.append(mm_nt(olb, vh).astype(BF))
        keep.append((ql, ol, olb, top + jnp.log(total)))
    o = jnp.concatenate(outs, -1)
    hres, b_all, fcols, drows = turn_forward(
        ns, nb, mm(o, wout).astype(BF), x, gain_f, fcols, w_down.astype(BF)
    )
    wgu = fcols.reshape(width, 2 * fl)
    wdown = drows.reshape(fl, width)
    gu = mm(b_all, wgu)
    gate, up = gu[:, :fl], gu[:, fl:]
    sig = jax.nn.sigmoid(gate)
    act = gate * sig
    hid = (act * up).astype(BF)
    part_y = mm(hid, wdown).astype(BF)

    dhid = mm_nt(dy_all, wdown)
    dgate = (dhid * up * sig * (1.0 + gate * (1.0 - sig))).astype(BF)
    dup = (dhid * act).astype(BF)
    dgu = jnp.concatenate([dgate, dup], -1)
    g_down = mm_tn(hid, dy_all).astype(BF).reshape(nb, fl // nb, width)
    g_gu = mm_tn(b_all, dgu).astype(BF).reshape(ns, nb, shard, 2 * fl)
    dres, dat_all, gg_f, g_gu, p_down = turn_back(
        ns, nb, mm_nt(dgu, wgu).astype(BF), gy, hres, gain_f, g_gu, g_down
    )
    g_out = mm_tn(o, dat_all)
    do = mm_nt(dat_all, wout).astype(BF)

    dqs, dqps, g_uk, g_uv = [], [], [], []
    dc = jnp.zeros((length, LAT), F32)
    dkr = jnp.zeros((length, ROPE), F32)
    for h in range(hl):
        ql, ol, olb, lse = keep[h]
        uh = ukey[h * HD : (h + 1) * HD]
        vh = uval[h * HD : (h + 1) * HD]
        doh = do[:, h * HD : (h + 1) * HD]
        g_uv.append(mm_tn(doh, olb))
        dol = mm(doh, vh).astype(BF)
        delta = jnp.sum(dol.astype(F32) * ol, -1, keepdims=True)
        sc = (mm_nt(ql, c) + mm_nt(qr[:, h], kr)) * scaling
        p = jnp.exp(jnp.where(causal, sc, NEG_FILL) - lse)
        ds = (p * (mm_nt(dol, c) - delta)).astype(BF)
        dql = (scaling * mm(ds, c)).astype(BF)
        dqps.append(rotate(scaling * mm(ds, kr), cosine, -sine).astype(BF))
        dkr = dkr + scaling * mm_tn(ds, qr[:, h])
        dc = dc + mm_tn(p.astype(BF), dol) + scaling * mm_tn(ds, ql)
        g_uk.append(mm_tn(q[:, h * HD : (h + 1) * HD], dql))
        dqs.append(mm_nt(dql, uh).astype(BF))
    dkp = rotate(dkr, cosine, -sine).astype(BF)
    gcat = jnp.concatenate(dqs + dqps + [dkp, jnp.zeros((length, PAD - ROPE), BF), dc.astype(BF)], -1)
    g_cat = mm_tn(a_all, gcat).astype(BF).reshape(ns, nb, shard, full)
    g_head = jnp.concatenate([jnp.concatenate(g_uk, 0), jnp.concatenate(g_uv, 0), g_out], -1)
    g_head = g_head.astype(BF).reshape(nb, shard, -1)
    dx, y, gg, r_cat, p_head, r_gu = settle(
        ns, nb, mm_nt(gcat, wcat).astype(BF), part_y, x, hres, dres, gain_a, gg_f, g_cat, g_head, g_gu
    )

    def spread(v):
        return v.transpose(1, 0, 2).reshape(shard, -1).astype(F32)

    group = ns // GROUPS
    p_latent = r_cat[:, :, lat_at:].astype(F32).reshape(GROUPS, group, shard, LAT).sum(1)
    gg = lax.dynamic_slice(gg, (0, (me * nb + bat) * shard), (2, shard))
    return (
        y.reshape(seq_count, rows, width),
        dx.reshape(seq_count, rows, width),
        gg[0],
        spread(r_cat[:, :, :qw]),
        spread(r_cat[:, :, qw : qw + rw]),
        spread(p_latent),
        r_cat[:, :, kr_at : kr_at + ROPE].astype(F32).sum(0),
        p_head[:, :LAT],
        p_head[:, LAT : 2 * LAT],
        p_head[:, 2 * LAT :],
        gg[1],
        spread(r_gu[:, :, :fl]),
        spread(r_gu[:, :, fl:]),
        p_down,
    )


def solution(mesh):
    token, row, flat = P("batch", "seq", None), P(("seq", "batch"), None), P(("seq", "batch"))
    return jax.shard_map(
        local,
        mesh=mesh,
        in_specs=(token, token, P("batch"), P(), flat, row, row, row, row, row, row, row, flat, row, row, row),
        out_specs=(token, token, flat, row, row, row, row, row, row, row, flat, row, row, row),
        check_vma=False,
    )
```

```python
import jax
import jax.numpy as jnp
from jax import lax
from jax.experimental import pallas as pl
from jax.experimental.pallas import tpu as pltpu
from jax.sharding import PartitionSpec as P

FF = 2816
H = 16
HD = 64
GROUPS = 2
LAT = 256
ROPE = 64
HALF = LAT // 2
ROWS = 256
SCALE = (HD + ROPE) ** (-0.5)

EPSILON = 1e-05
ROTARY_BASE = 10000.0
NEG_FILL = -1e30
WIDTH = 1024
BF = jnp.bfloat16
F32 = jnp.float32
MESH = pl.DeviceIdType.MESH
DMA = pltpu.SemaphoreType.DMA
VMEM = pl.BlockSpec(memory_space=pltpu.VMEM)


def mm(a, b):
    return jnp.dot(a, b, preferred_element_type=F32)


def mm_tn(a, b):
    return lax.dot_general(a, b, (((0,), (0,)), ((), ())), preferred_element_type=F32)


def mm_nt(a, b):
    return lax.dot_general(a, b, (((1,), (1,)), ((), ())), preferred_element_type=F32)


def rms(v, g):
    inv = lax.rsqrt(jnp.mean(v * v, -1, keepdims=True) + EPSILON)
    return inv, v * inv * g


def rms_grad(v, inv, g, dn):
    scaled = dn * g
    back = inv * scaled - v * (inv * inv * inv) * jnp.mean(scaled * v, -1, keepdims=True)
    return back, jnp.sum(dn * v * inv, 0, keepdims=True)


def rotate(v, cosine, sine):
    half = v.shape[-1] // 2
    lo, hi = v[..., :half], v[..., half:]
    return jnp.concatenate([lo * cosine - hi * sine, lo * sine + hi * cosine], -1)


def last(mask):
    return mask.bit_length() - 1


def aligned(start, size):
    return pl.ds(pl.multiple_of(start, size), size)


class Place:
    def __init__(self, ns, nb):
        self.ns, self.nb, self.nc = ns, nb, ns // 2
        self.dims = last(self.nc)
        self.me = lax.axis_index("seq")
        self.bat = lax.axis_index("batch")
        self.core = lax.rem(self.me, 2)
        self.chip = self.me // 2
        self.sib = self.chip * 2 + 1 - self.core

    def across(self, mask, core):
        spot = self.chip
        for j in range(self.dims):
            if mask >> j & 1:
                step = core * (1 << j) + (1 - core) * (1 << (self.dims - 1 - j))
                spot = spot + step - 2 * step * lax.rem(spot // step, 2)
        return spot * 2 + core

    def at(self, mask):
        return self.across(mask, self.core)

    def sib_at(self, mask):
        return self.across(mask, 1 - self.core)

    def seq(self, src, dst, send, recv, to):
        return pltpu.make_async_remote_copy(src, dst, send, recv, device_id={"seq": to}, device_id_type=MESH)

    def batch(self, src, dst, send, recv, to):
        return pltpu.make_async_remote_copy(src, dst, send, recv, device_id={"batch": to}, device_id_type=MESH)

    def barrier(self, all_seq, all_batch):
        sem = pltpu.get_barrier_semaphore()
        if all_seq:
            peers = [lax.rem(self.me + t, self.ns) for t in range(1, self.ns)]
        else:
            peers = [self.sib] + [self.at(1 << j) for j in range(self.dims)]
        for to in peers:
            pl.semaphore_signal(sem, 1, device_id={"seq": to}, device_id_type=MESH)
        count = len(peers)
        if all_batch:
            for t in range(1, self.nb):
                to = lax.rem(self.bat + t, self.nb)
                pl.semaphore_signal(sem, 1, device_id={"batch": to}, device_id_type=MESH)
            pl.semaphore_wait(sem, count + self.nb - 1)
            return

        @pl.when(self.bat > 0)
        def _():
            pl.semaphore_signal(sem, 1, device_id={"batch": self.bat - 1}, device_id_type=MESH)

        @pl.when(self.bat < self.nb - 1)
        def _():
            pl.semaphore_signal(sem, 1, device_id={"batch": self.bat + 1}, device_id_type=MESH)

        up = (self.bat > 0).astype(jnp.int32)
        down = (self.bat < self.nb - 1).astype(jnp.int32)
        pl.semaphore_wait(sem, count + up + down)


class Gather:
    def __init__(self, place, src, out, chunks, sems):
        self.place, self.src, self.out, self.chunks = place, src, out, chunks
        self.rows = src.shape[0]
        self.send, self.recv, self.sib_send, self.sib_recv = sems

    @staticmethod
    def sems(ns, chunks):
        nc = ns // 2
        hops, blocks = max(nc - 1, 1) * chunks, nc * chunks
        return [DMA((hops,)), DMA((hops,)), DMA((blocks,)), DMA((blocks,))]

    def slot(self, dev, ch):
        n = self.rows // self.chunks
        return self.out.at[pl.ds(pl.multiple_of(dev * self.rows + ch * n, n), n)]

    def block(self, mask, ch):
        n = self.rows // self.chunks
        if mask == 0:
            return self.src.at[pl.ds(ch * n, n)]
        return self.slot(self.place.at(mask), ch)

    def sends(self, mask, ch):
        place, copies = self.place, []
        for j in range(last(mask) + 1, place.dims):
            i = ((mask | 1 << j) - 1) * self.chunks + ch
            copies.append(
                place.seq(
                    self.block(mask, ch),
                    self.slot(place.at(mask), ch),
                    self.send.at[i],
                    self.recv.at[i],
                    place.at(1 << j),
                )
            )
        i = mask * self.chunks + ch
        copies.append(
            place.seq(
                self.block(mask, ch), self.slot(place.at(mask), ch), self.sib_send.at[i], self.sib_recv.at[i], place.sib
            )
        )
        return copies

    def start(self):
        for ch in range(self.chunks):
            for copy in self.sends(0, ch):
                copy.start()

    def relay(self, masks=None):
        place = self.place
        for mask in masks or range(1, place.nc):
            for ch in range(self.chunks):
                i = (mask - 1) * self.chunks + ch
                spot = self.slot(place.at(mask), ch)
                place.seq(spot, spot, self.send.at[i], self.recv.at[i], place.at(1 << last(mask))).wait_recv()
                for copy in self.sends(mask, ch):
                    copy.start()

    def finish(self):
        place = self.place
        for mask in range(place.nc):
            for ch in range(self.chunks):
                for copy in self.sends(mask, ch):
                    copy.wait_send()
                i = mask * self.chunks + ch
                spot = self.slot(place.sib_at(mask), ch)
                place.seq(spot, spot, self.sib_send.at[i], self.sib_recv.at[i], place.sib).wait_recv()


class Scatter:
    def __init__(self, place, part, bufs, sems):
        self.place, self.part = place, part
        self.acc, self.land, self.sib_land = bufs
        self.send, self.recv, self.sib_send, self.sib_recv = sems
        self.rows = part.shape[0] // place.ns

    @staticmethod
    def sems(ns):
        nc = ns // 2
        return [DMA((max(nc - 1, 1),)), DMA((max(nc - 1, 1),)), DMA((nc,)), DMA((nc,))]

    @staticmethod
    def bufs(ns, rows, width):
        return [pltpu.VMEM((ns // 2, rows, width), BF)] * 3

    def own(self, dev):
        return self.part.at[aligned(dev * self.rows, self.rows)]

    def sibling(self, mask):
        place = self.place
        return place.seq(
            self.own(place.sib_at(mask)),
            self.sib_land.at[mask],
            self.sib_send.at[mask],
            self.sib_recv.at[mask],
            place.sib,
        )

    def hop(self, mask):
        place = self.place
        return place.seq(
            self.acc.at[mask],
            self.land.at[mask],
            self.send.at[mask - 1],
            self.recv.at[mask - 1],
            place.at(1 << last(mask)),
        )

    def start(self):
        for mask in reversed(range(self.place.nc)):
            self.sibling(mask).start()

    def step(self, mask):
        place = self.place
        self.sibling(mask).wait_recv()
        value = self.own(place.at(mask))[...].astype(F32) + self.sib_land[mask].astype(F32)
        for j in reversed(range(last(mask) + 1, place.dims)):
            self.hop(mask | 1 << j).wait_recv()
            value = value + self.land[mask | 1 << j].astype(F32)
        if mask:
            self.acc[mask] = value.astype(BF)
            self.hop(mask).start()
        return value

    def total(self):
        for mask in reversed(range(1, self.place.nc)):
            self.step(mask)
        return self.step(0)

    def finish(self):
        for mask in range(self.place.nc):
            self.sibling(mask).wait_send()
            if mask:
                self.hop(mask).wait_send()


class Line:
    def __init__(self, place, slots, sems):
        self.place, self.slots = place, slots
        self.send, self.recv = sems

    @staticmethod
    def sems(nb, parts):
        return [DMA((2 * nb * parts,)), DMA((2 * nb * parts,))]

    def copy(self, up, d, i):
        place = self.place
        block = place.bat - d if up else place.bat + d
        to = place.bat + 1 if up else place.bat - 1
        ref = self.slots[i](block)
        at = (int(up) * place.nb + d) * len(self.slots) + i
        return place.batch(ref, ref, self.send.at[at], self.recv.at[at], to)

    def sends(self, up, d):
        bat, nb = self.place.bat, self.place.nb
        return (bat - d >= 0) & (bat + 1 < nb) if up else (bat + d < nb) & (bat >= 1)

    def start(self, d, parts):
        for up in (True, False):

            @pl.when(self.sends(up, d))
            def _(up=up):
                for i in parts:
                    self.copy(up, d, i).start()

    def came(self, up, d):
        return self.place.bat - d >= 0 if up else self.place.bat + d < self.place.nb

    def relay(self, d, parts, then=None):
        bat, nb = self.place.bat, self.place.nb
        for up in (True, False):

            @pl.when(self.came(up, d))
            def _(up=up):
                for i in parts:
                    block = bat - d if up else bat + d
                    ref = self.slots[i](block)
                    at = (int(up) * nb + d - 1) * len(self.slots) + i
                    self.place.batch(ref, ref, self.send.at[at], self.recv.at[at], bat).wait_recv()
                    if d < nb - 1:

                        @pl.when(self.sends(up, d))
                        def _():
                            self.copy(up, d, i).start()

                    if then:
                        then(block, up, i)

    def finish(self, parts):
        for d in range(self.place.nb - 1):
            for up in (True, False):

                @pl.when(self.sends(up, d))
                def _(up=up, d=d):
                    for i in parts:
                        self.copy(up, d, i).wait_send()


class LineSum:
    def __init__(self, place, parts, bufs, sems):
        self.place, self.parts = place, parts
        self.bufs = [bufs[4 * i : 4 * i + 4] for i in range(len(parts))]
        self.send, self.recv = sems

    @staticmethod
    def sems(nb, parts):
        return [DMA((2 * nb * parts,)), DMA((2 * nb * parts,))]

    @staticmethod
    def scratch(nb, shapes):
        slots = (nb - 1, nb - 2, nb - 1, nb - 2)
        return [pltpu.VMEM((n,) + shape, BF) for shape in shapes for n in slots]

    def copy(self, up, d, i, first):
        place = self.place
        land, acc = self.bufs[i][:2] if up else self.bufs[i][2:]
        to = place.bat + 1 if up else place.bat - 1
        dest = place.bat + d if up else place.bat - d
        src = self.parts[i](dest) if first else acc.at[d - 1]
        at = (int(up) * place.nb + d) * len(self.parts) + i
        return place.batch(src, land.at[d - 1], self.send.at[at], self.recv.at[at], to)

    def arrived(self, up, d, i):
        place = self.place
        land = self.bufs[i][0 if up else 2]
        at = (int(up) * place.nb + d + 1) * len(self.parts) + i
        place.batch(land.at[d], land.at[d], self.send.at[at], self.recv.at[at], place.bat).wait_recv()
        return land[d].astype(F32)

    def edge(self, up):
        return self.place.bat == 0 if up else self.place.bat == self.place.nb - 1

    def inside(self, up, d):
        return self.place.bat + d < self.place.nb if up else self.place.bat - d >= 0

    def start(self):
        for d in reversed(range(1, self.place.nb)):
            for up in (True, False):

                @pl.when(self.edge(up))
                def _(up=up, d=d):
                    for i in range(len(self.parts)):
                        self.copy(up, d, i, True).start()

    def stage(self, d):
        for up in (True, False):

            @pl.when(self.inside(up, d) & jnp.logical_not(self.edge(up)))
            def _(up=up):
                for i in range(len(self.parts)):
                    dest = self.place.bat + d if up else self.place.bat - d
                    acc = self.bufs[i][1 if up else 3]
                    acc[d - 1] = (self.parts[i](dest)[...].astype(F32) + self.arrived(up, d, i)).astype(BF)
                    self.copy(up, d, i, False).start()

    def total(self, outs):
        for i, out in enumerate(outs):
            out[...] = self.parts[i](self.place.bat)[...].astype(out.dtype)
            for up in (True, False):

                @pl.when(jnp.logical_not(self.edge(up)))
                def _(up=up):
                    out[...] = (out[...].astype(F32) + self.arrived(up, 0, i)).astype(out.dtype)

    def finish(self):
        for d in range(1, self.place.nb):
            for up in (True, False):

                @pl.when(self.inside(up, d) & self.edge(up))
                def _(up=up, d=d):
                    for i in range(len(self.parts)):
                        self.copy(up, d, i, True).wait_send()

                @pl.when(self.inside(up, d) & jnp.logical_not(self.edge(up)))
                def _(up=up, d=d):
                    for i in range(len(self.parts)):
                        self.copy(up, d, i, False).wait_send()


class Exchange:
    def __init__(self, place, pieces, slots, sems):
        self.place, self.pieces, self.slots = place, pieces, slots
        self.send, self.recv = sems

    @staticmethod
    def sems(ns, parts):
        return [DMA((ns * parts,)), DMA((ns * parts,))]

    def copy(self, t, i):
        place = self.place
        to = lax.rem(place.me + t, place.ns)
        at = t * len(self.pieces) + i
        src, dst = self.pieces[i](to), self.slots[i](place.me, to)
        if t == 0:
            return pltpu.make_async_copy(src, dst, self.recv.at[at])
        return place.seq(src, dst, self.send.at[at], self.recv.at[at], to)

    def start(self):
        for t in range(self.place.ns):
            for i in range(len(self.pieces)):
                self.copy(t, i).start()

    def arrive(self):
        place = self.place
        for t in range(place.ns):
            for i in range(len(self.pieces)):
                if t == 0:
                    self.copy(0, i).wait()
                    continue
                at = t * len(self.pieces) + i
                spot = self.slots[i](lax.rem(place.me + place.ns - t, place.ns), place.me)
                place.seq(spot, spot, self.send.at[at], self.recv.at[at], place.sib).wait_recv()

    def finish(self):
        for t in range(1, self.place.ns):
            for i in range(len(self.pieces)):
                self.copy(t, i).wait_send()


def take(refs, counts):
    out, at = [], 0
    for n in counts:
        out.append(refs[at : at + n])
        at += n
    return out


def comm_call(body, out_shape, scratch, cid, *args):
    return pl.pallas_call(
        body,
        out_shape=out_shape,
        in_specs=[VMEM] * len(args),
        out_specs=[VMEM] * len(out_shape),
        scratch_shapes=scratch,
        compiler_params=pltpu.CompilerParams(
            collective_id=cid, has_side_effects=True, vmem_limit_bytes=60 << 20
        ),
    )(*args)


def sds(shape, dtype):
    return jax.ShapeDtypeStruct(tuple(shape), dtype)


def half_of(v, h):
    lane = lax.broadcasted_iota(jnp.int32, v.shape, 1)
    return jnp.where(lane // HD == h, v, jnp.zeros_like(v))


def turn(v, cosine, sine):
    lane = lax.broadcasted_iota(jnp.int32, v.shape, 1)
    width, half = v.shape[1], ROPE // 2
    swapped = jnp.where((lane // half) % 2 == 0, pltpu.roll(v, width - half, 1), pltpu.roll(v, half, 1))
    return v * cosine + swapped * sine


def blocks(count, body):
    def step(i, carry):
        body(aligned(i * ROWS, ROWS))
        return carry

    lax.fori_loop(0, count, step, 0)


def normalize(r, x, gain, a):
    a[r, :] = rms(x[r, :].astype(F32), gain)[1].astype(BF)


def project(r, a, wcat, ukey, cosine, sine, q, qr, kr, c, ql):
    qkv = mm(a[r, :], wcat)
    co, si = cosine[r, :], sine[r, :]
    qt = qkv[:, :128].astype(BF)
    q[r, :] = qt
    qr[r, :] = turn(qkv[:, 128:256], co, si).astype(BF)
    kr[r, :] = turn(qkv[:, 256:384], co, si).astype(BF)
    c[r, :] = qkv[:, 384:].astype(BF)
    for h in range(2):
        ql[r, h * LAT : (h + 1) * LAT] = mm(half_of(qt, h), ukey).astype(BF)


def scores(i, h, q_lat, q_rope, c, kr):
    n = (i + 1) * ROWS
    s = (mm_nt(q_lat, c[:n, :]) + mm_nt(half_of(q_rope, h), kr[:n, :])) * SCALE
    row = lax.broadcasted_iota(jnp.int32, (ROWS, ROWS), 0)
    col = lax.broadcasted_iota(jnp.int32, (ROWS, ROWS), 1)
    own = jnp.where(col <= row, s[:, n - ROWS :], NEG_FILL)
    return own if i == 0 else jnp.concatenate([s[:, : n - ROWS], own], 1)


def attend(i, q_lat, q_rope, c, kr, uval, wout, ol, lse, o, part):
    n, r = (i + 1) * ROWS, pl.ds(i * ROWS, ROWS)
    outs = []
    for h in range(2):
        w = slice(h * LAT, (h + 1) * LAT)
        s = scores(i, h, q_lat[r, w], q_rope[r, :], c, kr)
        top = jnp.max(s, -1, keepdims=True)
        e = jnp.exp(s - top)
        total = jnp.sum(e, -1, keepdims=True)
        v = mm(e.astype(BF), c[:n, :]) / total
        ol[r, w] = v
        lse[h, r, :] = jnp.broadcast_to(top + jnp.log(total), (ROWS, 128))
        outs.append(half_of(mm_nt(v.astype(BF), uval), h))
    ot = (outs[0] + outs[1]).astype(BF)
    o[r, :] = ot
    part[r, :] = mm(ot, wout).astype(BF)


def attend_back(i, first, q_lat, q_rope, c, kr, uval, ukey, wout, ol, lse, o, q, dat, cosine, sine, dc, dk, sums, gcat):
    n, r = (i + 1) * ROWS, pl.ds(i * ROWS, ROWS)
    d = dat[r, :]
    do = mm_nt(d, wout).astype(BF)
    out_grad = mm_tn(o[r, :], d)
    qt = q[r, :]
    dq, dqr, uk, uv = 0.0, 0.0, 0.0, 0.0
    for h in range(2):
        w = slice(h * LAT, (h + 1) * LAT)
        doh = half_of(do, h)
        out = ol[r, w]
        uv = uv + mm_tn(doh, out.astype(BF))
        dol = mm(doh, uval).astype(BF)
        delta = jnp.sum(dol.astype(F32) * out, -1, keepdims=True)
        lat = q_lat[r, w]
        p = jnp.exp(scores(i, h, lat, q_rope[r, :], c, kr) - lse[h, r, :][:, :1])
        ds = (p * ((mm_nt(dol, c[:n, :]) - delta) * SCALE)).astype(BF)
        dql = mm(ds, c[:n, :]).astype(BF)
        dqr = dqr + half_of(mm(ds, kr[:n, :]), h)
        dc_new = mm_tn(jnp.concatenate([p.astype(BF), ds], 0), jnp.concatenate([dol, lat], 0))
        dk_new = mm_tn(ds, half_of(q_rope[r, :], h))
        if first and h == 0:
            dc[:n, :] = dc_new
            dk[:n, :] = dk_new
        else:
            dc[:n, :] += dc_new
            dk[:n, :] += dk_new
        uk = uk + mm_tn(half_of(qt, h), dql)
        dq = dq + half_of(mm_nt(dql, ukey), h)
    for ref, value in zip(sums, (uk, uv, out_grad)):
        if first:
            ref[...] = value
        else:
            ref[...] += value
    co, si = cosine[r, :], -sine[r, :]
    gcat[r, :128] = dq.astype(BF)
    gcat[r, 128:256] = turn(dqr, co, si).astype(BF)
    gcat[r, 256:384] = turn(dk[r, :], co, si).astype(BF)
    gcat[r, 384:] = dc[r, :].astype(BF)


def seq_gather(v):
    return lax.all_gather(v, "seq", axis=0, tiled=True)


def seq_sum(v):
    return lax.psum_scatter(v.astype(BF), "seq", scatter_dimension=0, tiled=True).astype(F32)


def batch_gather(v):
    return lax.all_gather(v, "batch", axis=0, tiled=True)


def batch_sum(v):
    return lax.psum_scatter(v.astype(BF), "batch", scatter_dimension=0, tiled=True).astype(F32)


def plain(
    tokens,
    out_grad,
    group_id,
    group_weight,
    gain_attn,
    w_query,
    w_qrope,
    w_latent,
    w_krope,
    w_ukey,
    w_uval,
    w_out,
    gain_ffn,
    w_gate,
    w_up,
    w_down,
):
    ns, nb = lax.axis_size("seq"), lax.axis_size("batch")
    seq_count, rows, width = tokens.shape
    shard = w_query.shape[0]
    length = rows * ns
    hl = H // ns
    fl = FF // ns
    qw, rw = hl * HD, hl * ROPE
    scaling = (HD + ROPE) ** (-0.5)

    def columns(w, blocks):
        return w.astype(BF).reshape(shard, blocks, -1).transpose(1, 0, 2)

    lat_cols = jnp.repeat(columns(w_latent, GROUPS), ns // GROUPS, axis=0)
    kr_cols = jnp.broadcast_to(w_krope.astype(BF)[None], (ns, shard, ROPE))
    send = jnp.concatenate(
        [columns(w_query, ns), columns(w_qrope, ns), lat_cols, kr_cols, columns(w_gate, ns), columns(w_up, ns)], -1
    )
    got = lax.all_to_all(send, "seq", 0, 0)
    wide = send.shape[-1]
    full = lax.all_gather(got, "batch", axis=1).reshape(width, wide)
    attn_w = qw + rw + LAT + ROPE
    wcat, wgu = full[:, :attn_w], full[:, attn_w:]
    ukey = batch_gather(w_ukey.astype(BF))
    uval = batch_gather(w_uval.astype(BF))
    wout = batch_gather(w_out.astype(BF))
    wdown = batch_gather(w_down.astype(BF))
    gains = lax.all_gather(
        jnp.stack([gain_attn, gain_ffn]).astype(BF), ("seq", "batch"), axis=1, tiled=True
    ).astype(F32)
    gain_a, gain_f = gains[0], gains[1]

    x = tokens.reshape(rows, width)
    domains = jnp.arange(group_weight.shape[0])
    seq_weight = jnp.sum(jnp.where(group_id[:, None] == domains[None, :], group_weight[None, :], 0.0), -1)
    gy = (out_grad.astype(F32) * seq_weight[:, None, None]).reshape(rows, width)
    dy_all = seq_gather(gy.astype(BF))
    x_all = seq_gather(x)
    x32 = x.astype(F32)

    position = jnp.arange(length).astype(F32)
    freq = ROTARY_BASE ** (-jnp.arange(ROPE // 2).astype(F32) * 2.0 / ROPE)
    angles = position[:, None] * freq
    cosine, sine = jnp.cos(angles), jnp.sin(angles)

    _, normed = rms(x_all.astype(F32), gain_a)
    a_all = normed.astype(BF)
    qkv = mm(a_all, wcat)
    q = qkv[:, :qw].astype(BF)
    qr = rotate(qkv[:, qw : qw + rw].reshape(length, hl, ROPE), cosine[:, None], sine[:, None]).astype(BF)
    c = qkv[:, qw + rw : qw + rw + LAT].astype(BF)
    kr = rotate(qkv[:, qw + rw + LAT :], cosine, sine).astype(BF)
    causal = jnp.arange(length)[None, :] <= jnp.arange(length)[:, None]

    keep = []
    outs = []
    for h in range(hl):
        uh = ukey[h * HD : (h + 1) * HD]
        vh = uval[h * HD : (h + 1) * HD]
        ql = mm(q[:, h * HD : (h + 1) * HD], uh).astype(BF)
        sc = (mm_nt(ql, c) + mm_nt(qr[:, h], kr)) * scaling
        sc = jnp.where(causal, sc, NEG_FILL)
        top = jnp.max(sc, -1, keepdims=True)
        e = jnp.exp(sc - top)
        total = jnp.sum(e, -1, keepdims=True)
        ol = mm(e.astype(BF), c) / total
        olb = ol.astype(BF)
        outs.append(mm_nt(olb, vh).astype(BF))
        keep.append((ql, ol, olb, top + jnp.log(total)))
    o = jnp.concatenate(outs, -1)
    hres = x32 + seq_sum(mm(o, wout))
    inv_f, normed_f = rms(hres, gain_f)
    b_all = seq_gather(normed_f.astype(BF))
    gu = mm(b_all, wgu)
    gate, up = gu[:, :fl], gu[:, fl:]
    sig = jax.nn.sigmoid(gate)
    act = gate * sig
    hid = (act * up).astype(BF)
    y = seq_sum(mm(hid, wdown))
    result = (hres + y).astype(BF).reshape(seq_count, rows, width)

    dhid = mm_nt(dy_all, wdown)
    dgate = (dhid * up * sig * (1.0 + gate * (1.0 - sig))).astype(BF)
    dup = (dhid * act).astype(BF)
    dgu = jnp.concatenate([dgate, dup], -1)
    db = seq_sum(mm_nt(dgu, wgu))
    g_down = batch_sum(mm_tn(hid, dy_all))
    g_gu = mm_tn(b_all, dgu)
    back_f, gg_f = rms_grad(hres, inv_f, gain_f, db)
    dres = gy + back_f
    dat_all = seq_gather(dres.astype(BF))
    g_out = mm_tn(o, dat_all)
    do = mm_nt(dat_all, wout).astype(BF)

    dqs, dqps, g_uk, g_uv = [], [], [], []
    dc = jnp.zeros((length, LAT), F32)
    dkr = jnp.zeros((length, ROPE), F32)
    for h in range(hl):
        ql, ol, olb, lse = keep[h]
        uh = ukey[h * HD : (h + 1) * HD]
        vh = uval[h * HD : (h + 1) * HD]
        doh = do[:, h * HD : (h + 1) * HD]
        g_uv.append(mm_tn(doh, olb))
        dol = mm(doh, vh).astype(BF)
        delta = jnp.sum(dol.astype(F32) * ol, -1, keepdims=True)
        sc = (mm_nt(ql, c) + mm_nt(qr[:, h], kr)) * scaling
        p = jnp.exp(jnp.where(causal, sc, NEG_FILL) - lse)
        ds = (p * (mm_nt(dol, c) - delta)).astype(BF)
        dql = (scaling * mm(ds, c)).astype(BF)
        dqps.append(rotate(scaling * mm(ds, kr), cosine, -sine).astype(BF))
        dkr = dkr + scaling * mm_tn(ds, qr[:, h])
        dc = dc + mm_tn(p.astype(BF), dol) + scaling * mm_tn(ds, ql)
        g_uk.append(mm_tn(q[:, h * HD : (h + 1) * HD], dql))
        dqs.append(mm_nt(dql, uh).astype(BF))
    dkp = rotate(dkr, cosine, -sine).astype(BF)
    gcat = jnp.concatenate(dqs + dqps + [dc.astype(BF), dkp], -1)
    da = seq_sum(mm_nt(gcat, wcat))
    g_cat = mm_tn(a_all, gcat)
    inv_a, _ = rms(x32, gain_a)
    back_a, gg_a = rms_grad(x32, inv_a, gain_a, da)
    input_grad = (dres + back_a).reshape(seq_count, rows, width)

    def wide_sum(g):
        cols = g.shape[-1]
        part = lax.psum_scatter(
            g.astype(BF).reshape(ns, nb, shard, cols), "batch", scatter_dimension=1, tiled=True
        ).reshape(ns, shard, cols)
        return lax.all_to_all(part, "seq", 0, 0)

    def spread(v):
        return v.transpose(1, 0, 2).reshape(shard, -1)

    r_gu = wide_sum(g_gu)
    r_cat = wide_sum(g_cat).astype(F32)
    p_query = spread(r_cat[:, :, :qw])
    p_qrope = spread(r_cat[:, :, qw : qw + rw])
    p_latent = spread(
        r_cat[:, :, qw + rw : qw + rw + LAT].reshape(GROUPS, ns // GROUPS, shard, LAT).sum(1)
    )
    p_krope = r_cat[:, :, qw + rw + LAT :].sum(0)
    p_gate = spread(r_gu[:, :, :fl]).astype(F32)
    p_up = spread(r_gu[:, :, fl:]).astype(F32)
    g_head = batch_sum(jnp.concatenate([jnp.concatenate(g_uk, 0), jnp.concatenate(g_uv, 0), g_out], -1))
    gg = lax.psum_scatter(jnp.concatenate([gg_a, gg_f]), ("seq", "batch"), scatter_dimension=1, tiled=True)
    return (
        result,
        input_grad,
        gg[0],
        p_query,
        p_qrope,
        p_latent,
        p_krope,
        g_head[:, :LAT],
        g_head[:, LAT : 2 * LAT],
        g_head[:, 2 * LAT :],
        gg[1],
        p_gate,
        p_up,
        g_down,
    )


class Total:
    def __init__(self, place, own, by_seq, by_batch, sems):
        self.place, self.own, self.by_seq, self.by_batch = place, own, by_seq, by_batch
        self.over = Exchange(place, [lambda to: own], [lambda frm, to: by_seq.at[frm]], sems[:2])
        self.send, self.recv = sems[2:]

    @staticmethod
    def scratch(ns, nb, shape):
        return [pltpu.VMEM(shape, F32), pltpu.VMEM((ns,) + shape, F32), pltpu.VMEM((nb,) + shape, F32)]

    @staticmethod
    def sems(ns, nb):
        return Exchange.sems(ns, 1) + [DMA((nb,)), DMA((nb,))]

    def start(self):
        self.over.start()

    def copy(self, t):
        place = self.place
        to = lax.rem(place.bat + t, place.nb)
        return place.batch(self.own, self.by_batch.at[place.bat], self.send.at[t], self.recv.at[t], to)

    def middle(self):
        self.over.arrive()
        self.over.finish()
        self.own[...] = jnp.sum(self.by_seq[...], 0)
        for t in range(1, self.place.nb):
            self.copy(t).start()
        self.by_batch[self.place.bat] = self.own[...]

    def result(self):
        place = self.place
        for t in range(1, place.nb):
            spot = self.by_batch.at[lax.rem(place.bat + place.nb - t, place.nb)]
            place.batch(spot, spot, self.send.at[t], self.recv.at[t], place.bat).wait_recv()
        return jnp.sum(self.by_batch[...], 0)

    def finish(self):
        for t in range(1, self.place.nb):
            self.copy(t).wait_send()


def forward(ns, nb, x, dy, wide_a, wide_f, head_rows, down, gains, cosine, sine, chunks=4):
    rows, width = x.shape
    length = ns * rows
    shard, aw = wide_a.shape[1:]
    qk = aw - HALF
    full = qk + LAT

    def body(x, dy, wa, wf, hr, dn, gin, co, si, *rest):
        outs, rest = rest[:17], rest[17:]
        dy_all, a_all, wc, hrow, fcol, drow, q, qr, kr, c, ql, ol, lse, o, hres, b_all, gout = outs
        x_all, part, own = rest[:3]
        bufs, tot, gx, gd, ea, ef, zl, zf, sib, rs, gs, ts, local = take(
            rest[3:], (3, 3, 4, 4, 2, 2, 2, 2, 2, 4, 4, 4, 1)
        )
        place = Place(ns, nb)
        local = local[0]
        mine = aligned(place.me * rows, rows)
        copies = [
            pltpu.make_async_copy(hr, hrow.at[place.bat], local.at[0]),
            pltpu.make_async_copy(x, x_all.at[mine], local.at[1]),
            pltpu.make_async_copy(dy, dy_all.at[mine], local.at[2]),
            pltpu.make_async_copy(dn, drow.at[place.bat], local.at[3]),
        ]
        for copy in copies:
            copy.start()
        gain = Total(place, *tot, ts)
        gain.own[...] = gin[...]
        place.barrier(True, True)

        def half(core):
            return pl.ds(pl.multiple_of(qk + HALF * core, HALF), HALF)

        cols = Exchange(
            place,
            [lambda to: wa.at[to, :, pl.ds(0, qk)], lambda to: wa.at[to, :, pl.ds(qk, HALF)]],
            [
                lambda frm, to: wc.at[frm, place.bat, :, pl.ds(0, qk)],
                lambda frm, to: wc.at[frm, place.bat, :, half(lax.rem(to, 2))],
            ],
            ea,
        )
        ffn = Exchange(place, [lambda to: wf.at[to]], [lambda frm, to: fcol.at[frm, place.bat]], ef)
        along = Line(
            place,
            [
                lambda b: hrow.at[b],
                lambda b: wc.at[:, b, :, pl.ds(0, qk)],
                lambda b: wc.at[:, b, :, half(place.core)],
            ],
            zl,
        )
        later = Line(place, [lambda b: fcol.at[:, b], lambda b: drow.at[b]], zf)

        def to_sibling(b, i):
            ref = wc.at[:, b, :, half(place.core)]
            return place.seq(ref, ref, sib[0].at[i], sib[1].at[i], place.sib)

        def from_sibling(b, i):
            ref = wc.at[:, b, :, half(1 - place.core)]
            place.seq(ref, ref, sib[0].at[i], sib[1].at[i], place.sib).wait_recv()

        def pass_on(d):
            along.relay(d, [0, 1])
            along.relay(d, [2], lambda b, up, i: to_sibling(b, d if up else nb - 1 + d).start())

        xs, ds = Gather(place, x, x_all, chunks, gx), Gather(place, dy, dy_all, chunks, gd)
        cols.start()
        copies[0].wait()
        along.start(0, [0])
        gain.start()
        xs.start()
        cols.arrive()
        along.start(0, [1, 2])
        to_sibling(place.bat, 0).start()
        gain.middle()
        xs.relay()
        ffn.start()
        ds.start()
        pass_on(1)
        gout[...] = gain.result()
        copies[1].wait()
        xs.finish()
        blocks(length // ROWS, lambda r: normalize(r, x_all, gout[pl.ds(0, 1), :], a_all))
        pass_on(2)
        ffn.arrive()
        copies[3].wait()
        later.start(0, [0, 1])
        for d in range(3, nb):
            pass_on(d)
        from_sibling(place.bat, 0)
        for d in range(1, nb):
            for up in (True, False):

                @pl.when(along.came(up, d))
                def _(up=up, d=d):
                    from_sibling(place.bat - d if up else place.bat + d, d if up else nb - 1 + d)

        ds.relay()
        wcat = wc[...].reshape(width, full)
        heads = hrow[...].reshape(nb * shard, head_rows.shape[1])
        ukey, uval, wout = heads[:, :LAT], heads[:, LAT : 2 * LAT], heads[:, 2 * LAT :]
        blocks(length // ROWS, lambda r: project(r, a_all, wcat, ukey, co, si, q, qr, kr, c, ql))
        for i in range(length // ROWS):
            attend(i, ql, qr, c, kr, uval, wout, ol, lse, o, part)
        sums = Scatter(place, part, bufs, rs)
        sums.start()
        later.relay(1, [0, 1])
        value = x[...].astype(F32) + sums.total()
        hres[...] = value
        own[...] = rms(value, gout[pl.ds(1, 1), :])[1].astype(BF)
        spread = Gather(place, own, b_all, chunks, gs)
        spread.start()
        last_copy = pltpu.make_async_copy(own, b_all.at[mine], local.at[4])
        last_copy.start()
        later.relay(2, [0, 1])
        spread.relay()
        for d in range(3, nb):
            later.relay(d, [0, 1])
        spread.finish()
        sums.finish()
        ds.finish()
        cols.finish()
        ffn.finish()
        along.finish([0, 1, 2])
        later.finish([0, 1])
        gain.finish()
        to_sibling(place.bat, 0).wait_send()
        for d in range(1, nb):
            for up in (True, False):

                @pl.when(along.came(up, d))
                def _(up=up, d=d):
                    to_sibling(place.bat - d if up else place.bat + d, d if up else nb - 1 + d).wait_send()

        copies[2].wait()
        last_copy.wait()

    scratch = (
        [pltpu.VMEM((length, width), BF), pltpu.VMEM((length, width), BF), pltpu.VMEM((rows, width), BF)]
        + Scatter.bufs(ns, rows, width)
        + Total.scratch(ns, nb, (2, width))
        + Gather.sems(ns, chunks)
        + Gather.sems(ns, chunks)
        + Exchange.sems(ns, 2)
        + Exchange.sems(ns, 1)
        + Line.sems(nb, 3)
        + Line.sems(nb, 2)
        + [DMA((2 * nb,)), DMA((2 * nb,))]
        + Scatter.sems(ns)
        + Gather.sems(ns, chunks)
        + Total.sems(ns, nb)
        + [DMA((5,))]
    )
    return comm_call(
        body,
        [
            sds((length, width), BF),
            sds((length, width), BF),
            sds((ns, nb, shard, full), BF),
            sds((nb,) + head_rows.shape, BF),
            sds((ns, nb) + wide_f.shape[1:], BF),
            sds((nb,) + down.shape, BF),
            sds((length, 128), BF),
            sds((length, 128), BF),
            sds((length, 128), BF),
            sds((length, LAT), BF),
            sds((length, 2 * LAT), BF),
            sds((length, 2 * LAT), F32),
            sds((2, length, 128), F32),
            sds((length, 128), BF),
            sds((rows, width), F32),
            sds((length, width), BF),
            sds((2, width), F32),
        ],
        scratch,
        1,
        x,
        dy,
        wide_a,
        wide_f,
        head_rows,
        down,
        gains,
        cosine,
        sine,
    )


def backward(ns, nb, part_db, part_y, gy, hres, x, gains, g_wide, g_down, saved, chunks=4):
    rows, width = x.shape
    length = ns * rows
    shard = g_wide.shape[2]
    full = saved[1].shape[-1]
    head_w = saved[2].shape[-1]
    block = (ns, shard, full)

    def body(pdb, py, gy, hres, x, gains, gw, gd, a_all, wc, hrow, q, qr, kr, c, ql, ol, lse, o, co, si, *rest):
        dx, y, gg, c_out, r_out, w_out, d_out = rest[:7]
        own, dres, dat_all, pda, dc, dk, uk, uv, og, gcat, gc, gr, c_sum, w_sum = rest[7:21]
        bd, by, ba, zfb, zab, tot, rd, ry, ra, gs, zf, za, ec, ew, ts, local = take(
            rest[21:], (3, 3, 3, 8, 8, 3, 4, 4, 4, 4, 2, 2, 2, 2, 4, 1)
        )
        place = Place(ns, nb)
        gain_a, gain_f = gains[pl.ds(0, 1), :], gains[pl.ds(1, 1), :]
        place.barrier(True, True)
        sums = Scatter(place, pdb, bd, rd)
        outs = Scatter(place, py, by, ry)
        later = LineSum(place, [lambda b: gw.at[:, b], lambda b: gd.at[b]], zfb, zf)
        sums.start()
        later.start()
        db = sums.total()
        value = hres[...]
        back, gg_f = rms_grad(value, rms(value, gain_f)[0], gain_f, db)
        value = gy[...] + back
        dres[...] = value
        own[...] = value.astype(BF)
        spread = Gather(place, own, dat_all, chunks, gs)
        spread.start()
        copy = pltpu.make_async_copy(own, dat_all.at[aligned(place.me * rows, rows)], local[0].at[0])
        copy.start()
        for d in reversed(range(2, nb - 1)):
            later.stage(d)
        spread.relay()
        outs.start()
        copy.wait()
        spread.finish()
        wcat = wc[...].reshape(width, full)
        heads = hrow[...].reshape(nb * shard, head_w)
        ukey, uval, wout = heads[:, :LAT], heads[:, LAT : 2 * LAT], heads[:, 2 * LAT :]
        wide = Exchange(place, [lambda to: w_sum.at[to]], [lambda frm, to: w_out.at[frm]], ew)
        count = length // ROWS
        todo = list(reversed(range(1, place.nc)))
        for i in reversed(range(count)):
            attend_back(
                i, i == count - 1, ql, qr, c, kr, uval, ukey, wout, ol, lse, o, q, dat_all, co, si, dc, dk, (uk, uv, og), gcat
            )
            if i == count - 1:
                later.stage(1)
            if todo:
                outs.step(todo.pop(0))
        for mask in todo:
            outs.step(mask)
        for j in range(ns):
            g = mm_tn(a_all[:, j * nb * shard : (j + 1) * nb * shard], gcat[...])
            gc[j] = g.astype(BF).reshape(nb, shard, full)
        heads_grad = jnp.concatenate([uk[...], uv[...], og[...]], 1)
        gr[...] = heads_grad.astype(BF).reshape(nb, shard, head_w)
        along = LineSum(place, [lambda b: gc.at[:, b], lambda b: gr.at[b]], zab, za)
        along.start()

        def da_block(r):
            pda[r, :] = mm_nt(gcat[r, :], wcat).astype(BF)

        blocks(count, da_block)
        ins = Scatter(place, pda, ba, ra)
        ins.start()
        later.total([w_sum, d_out])
        wide.start()
        y[...] = (hres[...] + outs.step(0)).astype(BF)
        for d in reversed(range(2, nb - 1)):
            along.stage(d)
        da = ins.total()
        value = x[...].astype(F32)
        back, gg_a = rms_grad(value, rms(value, gain_a)[0], gain_a, da)
        dx[...] = dres[...] + back
        gain = Total(place, *tot, ts)
        gain.own[pl.ds(0, 1), :] = gg_a
        gain.own[pl.ds(1, 1), :] = gg_f
        gain.start()
        along.stage(1)
        gain.middle()
        along.total([c_sum, r_out])
        cols = Exchange(place, [lambda to: c_sum.at[to]], [lambda frm, to: c_out.at[frm]], ec)
        cols.start()
        gg[...] = gain.result()
        wide.arrive()
        cols.arrive()
        for job in (gain, sums, outs, ins, later, along, wide, cols):
            job.finish()

    scratch = (
        [
            pltpu.VMEM((rows, width), BF),
            pltpu.VMEM((rows, width), F32),
            pltpu.VMEM((length, width), BF),
            pltpu.VMEM((length, width), BF),
            pltpu.VMEM((length, LAT), F32),
            pltpu.VMEM((length, 128), F32),
            pltpu.VMEM((128, LAT), F32),
            pltpu.VMEM((128, LAT), F32),
            pltpu.VMEM((128, width), F32),
            pltpu.VMEM((length, full), BF),
            pltpu.VMEM((ns, nb, shard, full), BF),
            pltpu.VMEM((nb, shard, head_w), BF),
            pltpu.VMEM(block, BF),
            pltpu.VMEM((ns,) + g_wide.shape[2:], BF),
        ]
        + Scatter.bufs(ns, rows, width) * 3
        + LineSum.scratch(nb, [(ns,) + g_wide.shape[2:], g_down.shape[1:]])
        + LineSum.scratch(nb, [block, (shard, head_w)])
        + Total.scratch(ns, nb, (2, width))
        + Scatter.sems(ns) * 3
        + Gather.sems(ns, chunks)
        + LineSum.sems(nb, 2)
        + LineSum.sems(nb, 2)
        + Exchange.sems(ns, 1)
        + Exchange.sems(ns, 1)
        + Total.sems(ns, nb)
        + [DMA((1,))]
    )
    return comm_call(
        body,
        [
            sds((rows, width), F32),
            sds((rows, width), BF),
            sds((2, width), F32),
            sds(block, BF),
            sds((shard, head_w), F32),
            sds((ns,) + g_wide.shape[2:], BF),
            sds(g_down.shape[1:], F32),
        ],
        scratch,
        2,
        part_db,
        part_y,
        gy,
        hres,
        x,
        gains,
        g_wide,
        g_down,
        *saved,
    )


def local(
    tokens,
    out_grad,
    group_id,
    group_weight,
    gain_attn,
    w_query,
    w_qrope,
    w_latent,
    w_krope,
    w_ukey,
    w_uval,
    w_out,
    gain_ffn,
    w_gate,
    w_up,
    w_down,
):
    ns, nb = lax.axis_size("seq"), lax.axis_size("batch")
    me, bat = lax.axis_index("seq"), lax.axis_index("batch")
    seq_count, rows, width = tokens.shape
    shard = w_query.shape[0]
    length = rows * ns
    fl = FF // ns
    qw = 2 * HD

    x = tokens.reshape(rows, width)
    domains = jnp.arange(group_weight.shape[0])
    seq_weight = jnp.sum(jnp.where(group_id[:, None] == domains[None, :], group_weight[None, :], 0.0), -1)
    gy = (out_grad.astype(F32) * seq_weight[:, None, None]).reshape(rows, width)

    def columns(w, count):
        return w.astype(BF).reshape(shard, count, -1).transpose(1, 0, 2)

    kr_cols = jnp.broadcast_to(jnp.tile(w_krope.astype(BF), (1, 2))[None], (ns, shard, 2 * ROPE))
    lat = columns(w_latent, GROUPS * 2).reshape(GROUPS, 1, 2, shard, HALF)
    lat = jnp.broadcast_to(lat, (GROUPS, ns // GROUPS // 2, 2, shard, HALF)).reshape(ns, shard, HALF)
    wide_a = jnp.concatenate([columns(w_query, ns), columns(w_qrope, ns), kr_cols, lat], -1)
    wide_f = jnp.concatenate([columns(w_gate, ns), columns(w_up, ns)], -1)
    head_rows = jnp.concatenate([w_ukey, w_uval, w_out], 1).astype(BF)
    gains = jnp.stack([gain_attn, gain_ffn]).astype(BF).astype(F32)
    first_row = (me * nb + bat) * shard
    gains = lax.dynamic_update_slice(jnp.zeros((2, width), F32), gains, (0, first_row))

    position = jnp.arange(length).astype(F32)
    freq = ROTARY_BASE ** (-jnp.arange(ROPE // 2).astype(F32) * 2.0 / ROPE)
    angles = position[:, None] * freq
    cosine, sine = jnp.cos(angles), jnp.sin(angles)
    cosine = jnp.tile(cosine, (1, 4))
    sine = jnp.tile(jnp.concatenate([-sine, sine], 1), (1, 2))

    (dy_all, a_all, wc, hrow, fcol, drow, q, qr, kr, c, ql, ol, lse, o, hres, b_all, gains) = forward(
        ns, nb, x, gy.astype(BF), wide_a, wide_f, head_rows, w_down.astype(BF), gains, cosine, sine
    )
    wgu = fcol.reshape(width, 2 * fl)
    wdown = drow.reshape(fl, width)
    gu = mm(b_all, wgu)
    gate, up = gu[:, :fl], gu[:, fl:]
    sig = jax.nn.sigmoid(gate)
    act = gate * sig
    hid = (act * up).astype(BF)
    part_y = mm(hid, wdown).astype(BF)
    dhid = mm_nt(dy_all, wdown)
    dgate = (dhid * up * sig * (1.0 + gate * (1.0 - sig))).astype(BF)
    dup = (dhid * act).astype(BF)
    dgu = jnp.concatenate([dgate, dup], -1)
    g_down = mm_tn(hid, dy_all).astype(BF).reshape(nb, fl // nb, width)
    g_gu = mm_tn(b_all, dgu).astype(BF).reshape(ns, nb, shard, 2 * fl)
    part_db = mm_nt(dgu, wgu).astype(BF)

    dx, y, gg, r_cat, p_head, r_gu, p_down = backward(
        ns,
        nb,
        part_db,
        part_y,
        gy,
        hres,
        x,
        gains,
        g_gu,
        g_down,
        (a_all, wc, hrow, q, qr, kr, c, ql, ol, lse, o, cosine, sine),
    )

    def spread(v):
        return v.transpose(1, 0, 2).reshape(shard, -1).astype(F32)

    p_latent = r_cat[:, :, 2 * qw + 2 * ROPE :]
    p_latent = p_latent.astype(F32).reshape(GROUPS, ns // GROUPS, shard, LAT).sum(1)
    p_krope = r_cat[:, :, 2 * qw : 2 * qw + 2 * ROPE].astype(F32).sum(0)
    gg = lax.dynamic_slice(gg, (0, first_row), (2, shard))
    return (
        y.reshape(seq_count, rows, width),
        dx.reshape(seq_count, rows, width),
        gg[0],
        spread(r_cat[:, :, :qw]),
        spread(r_cat[:, :, qw : 2 * qw]),
        spread(p_latent),
        p_krope[:, :ROPE] + p_krope[:, ROPE:],
        p_head[:, :LAT],
        p_head[:, LAT : 2 * LAT],
        p_head[:, 2 * LAT :],
        gg[1],
        spread(r_gu[:, :, :fl]),
        spread(r_gu[:, :, fl:]),
        p_down,
    )


def solution(mesh):
    token, row, flat = P("batch", "seq", None), P(("seq", "batch"), None), P(("seq", "batch"))
    ns, nb = mesh.shape["seq"], mesh.shape["batch"]
    fits = H == 2 * ns and (WIDTH // (ns * nb)) % 16 == 0 and nb > 2
    return jax.shard_map(
        local if fits else plain,
        mesh=mesh,
        in_specs=(token, token, P("batch"), P(), flat, row, row, row, row, row, row, row, flat, row, row, row),
        out_specs=(token, token, flat, row, row, row, row, row, row, row, flat, row, row, row),
        check_vma=False,
    )
```

```python
import jax
import jax.numpy as jnp
import numpy as np
from jax import lax
from jax.experimental import pallas as pl
from jax.experimental.pallas import tpu as pltpu
from jax.sharding import PartitionSpec as P

FF = 2816
H = 16
HD = 64
GROUPS = 2
LAT = 256
ROPE = 64
HALF = LAT // 2
ROWS = 256
SCALE = (HD + ROPE) ** (-0.5)

EPSILON = 1e-05
ROTARY_BASE = 10000.0
NEG_FILL = -1e30
WIDTH = 1024
BF = jnp.bfloat16
F32 = jnp.float32
MESH = pl.DeviceIdType.MESH
DMA = pltpu.SemaphoreType.DMA
VMEM = pl.BlockSpec(memory_space=pltpu.VMEM)


def mm(a, b):
    return jnp.dot(a, b, preferred_element_type=F32)


def mm_tn(a, b):
    return lax.dot_general(a, b, (((0,), (0,)), ((), ())), preferred_element_type=F32)


def mm_nt(a, b):
    return lax.dot_general(a, b, (((1,), (1,)), ((), ())), preferred_element_type=F32)


def rms(v, g):
    inv = lax.rsqrt(jnp.mean(v * v, -1, keepdims=True) + EPSILON)
    return inv, v * inv * g


def rms_grad(v, inv, g, dn):
    scaled = dn * g
    back = inv * scaled - v * (inv * inv * inv) * jnp.mean(scaled * v, -1, keepdims=True)
    return back, jnp.sum(dn * v * inv, 0, keepdims=True)


def rotate(v, cosine, sine):
    half = v.shape[-1] // 2
    lo, hi = v[..., :half], v[..., half:]
    return jnp.concatenate([lo * cosine - hi * sine, lo * sine + hi * cosine], -1)


def last(mask):
    return mask.bit_length() - 1


def aligned(start, size):
    return pl.ds(pl.multiple_of(start, size), size)


class Place:
    def __init__(self, ns, nb):
        self.ns, self.nb, self.nc = ns, nb, ns // 2
        self.dims = last(self.nc)
        self.me = lax.axis_index("seq")
        self.bat = lax.axis_index("batch")
        self.core = lax.rem(self.me, 2)
        self.chip = self.me // 2
        self.sib = self.chip * 2 + 1 - self.core

    def across(self, mask, core):
        spot = self.chip
        for j in range(self.dims):
            if mask >> j & 1:
                step = core * (1 << j) + (1 - core) * (1 << (self.dims - 1 - j))
                spot = spot + step - 2 * step * lax.rem(spot // step, 2)
        return spot * 2 + core

    def at(self, mask):
        return self.across(mask, self.core)

    def sib_at(self, mask):
        return self.across(mask, 1 - self.core)

    def seq(self, src, dst, send, recv, to):
        return pltpu.make_async_remote_copy(src, dst, send, recv, device_id={"seq": to}, device_id_type=MESH)

    def batch(self, src, dst, send, recv, to):
        return pltpu.make_async_remote_copy(src, dst, send, recv, device_id={"batch": to}, device_id_type=MESH)

    def barrier(self, all_seq, all_batch):
        sem = pltpu.get_barrier_semaphore()
        if all_seq:
            peers = [lax.rem(self.me + t, self.ns) for t in range(1, self.ns)]
        else:
            peers = [self.sib] + [self.at(1 << j) for j in range(self.dims)]
        for to in peers:
            pl.semaphore_signal(sem, 1, device_id={"seq": to}, device_id_type=MESH)
        count = len(peers)
        if all_batch:
            for t in range(1, self.nb):
                to = lax.rem(self.bat + t, self.nb)
                pl.semaphore_signal(sem, 1, device_id={"batch": to}, device_id_type=MESH)
            pl.semaphore_wait(sem, count + self.nb - 1)
            return

        @pl.when(self.bat > 0)
        def _():
            pl.semaphore_signal(sem, 1, device_id={"batch": self.bat - 1}, device_id_type=MESH)

        @pl.when(self.bat < self.nb - 1)
        def _():
            pl.semaphore_signal(sem, 1, device_id={"batch": self.bat + 1}, device_id_type=MESH)

        up = (self.bat > 0).astype(jnp.int32)
        down = (self.bat < self.nb - 1).astype(jnp.int32)
        pl.semaphore_wait(sem, count + up + down)


class Gather:
    def __init__(self, place, src, out, chunks, sems):
        self.place, self.src, self.out, self.chunks = place, src, out, chunks
        self.rows = src.shape[0]
        self.send, self.recv, self.sib_send, self.sib_recv = sems

    @staticmethod
    def sems(ns, chunks):
        nc = ns // 2
        hops, blocks = max(nc - 1, 1) * chunks, nc * chunks
        return [DMA((hops,)), DMA((hops,)), DMA((blocks,)), DMA((blocks,))]

    def slot(self, dev, ch):
        n = self.rows // self.chunks
        return self.out.at[pl.ds(pl.multiple_of(dev * self.rows + ch * n, n), n)]

    def block(self, mask, ch):
        n = self.rows // self.chunks
        if mask == 0:
            return self.src.at[pl.ds(ch * n, n)]
        return self.slot(self.place.at(mask), ch)

    def sends(self, mask, ch):
        place, copies = self.place, []
        for j in range(last(mask) + 1, place.dims):
            i = ((mask | 1 << j) - 1) * self.chunks + ch
            copies.append(
                place.seq(
                    self.block(mask, ch),
                    self.slot(place.at(mask), ch),
                    self.send.at[i],
                    self.recv.at[i],
                    place.at(1 << j),
                )
            )
        i = mask * self.chunks + ch
        copies.append(
            place.seq(
                self.block(mask, ch), self.slot(place.at(mask), ch), self.sib_send.at[i], self.sib_recv.at[i], place.sib
            )
        )
        return copies

    def start(self):
        for ch in range(self.chunks):
            for copy in self.sends(0, ch):
                copy.start()

    def relay(self, masks=None):
        place = self.place
        for mask in masks or range(1, place.nc):
            for ch in range(self.chunks):
                i = (mask - 1) * self.chunks + ch
                spot = self.slot(place.at(mask), ch)
                place.seq(spot, spot, self.send.at[i], self.recv.at[i], place.at(1 << last(mask))).wait_recv()
                for copy in self.sends(mask, ch):
                    copy.start()

    def finish(self):
        place = self.place
        for mask in range(place.nc):
            for ch in range(self.chunks):
                for copy in self.sends(mask, ch):
                    copy.wait_send()
                i = mask * self.chunks + ch
                spot = self.slot(place.sib_at(mask), ch)
                place.seq(spot, spot, self.sib_send.at[i], self.sib_recv.at[i], place.sib).wait_recv()


class Scatter:
    def __init__(self, place, part, bufs, sems):
        self.place, self.part = place, part
        self.acc, self.land, self.sib_land = bufs
        self.send, self.recv, self.sib_send, self.sib_recv = sems
        self.rows = part.shape[0] // place.ns

    @staticmethod
    def sems(ns):
        nc = ns // 2
        return [DMA((max(nc - 1, 1),)), DMA((max(nc - 1, 1),)), DMA((nc,)), DMA((nc,))]

    @staticmethod
    def bufs(ns, rows, width):
        return [pltpu.VMEM((ns // 2, rows, width), BF)] * 3

    def own(self, dev):
        return self.part.at[aligned(dev * self.rows, self.rows)]

    def sibling(self, mask):
        place = self.place
        return place.seq(
            self.own(place.sib_at(mask)),
            self.sib_land.at[mask],
            self.sib_send.at[mask],
            self.sib_recv.at[mask],
            place.sib,
        )

    def hop(self, mask):
        place = self.place
        return place.seq(
            self.acc.at[mask],
            self.land.at[mask],
            self.send.at[mask - 1],
            self.recv.at[mask - 1],
            place.at(1 << last(mask)),
        )

    def start(self):
        for mask in reversed(range(self.place.nc)):
            self.sibling(mask).start()

    def step(self, mask):
        place = self.place
        self.sibling(mask).wait_recv()
        value = self.own(place.at(mask))[...].astype(F32) + self.sib_land[mask].astype(F32)
        for j in reversed(range(last(mask) + 1, place.dims)):
            self.hop(mask | 1 << j).wait_recv()
            value = value + self.land[mask | 1 << j].astype(F32)
        if mask:
            self.acc[mask] = value.astype(BF)
            self.hop(mask).start()
        return value

    def total(self):
        for mask in reversed(range(1, self.place.nc)):
            self.step(mask)
        return self.step(0)

    def finish(self):
        for mask in range(self.place.nc):
            self.sibling(mask).wait_send()
            if mask:
                self.hop(mask).wait_send()


class Line:
    def __init__(self, place, slots, sems):
        self.place, self.slots = place, slots
        self.send, self.recv = sems

    @staticmethod
    def sems(nb, parts):
        return [DMA((2 * nb * parts,)), DMA((2 * nb * parts,))]

    def copy(self, up, d, i):
        place = self.place
        block = place.bat - d if up else place.bat + d
        to = place.bat + 1 if up else place.bat - 1
        ref = self.slots[i](block)
        at = (int(up) * place.nb + d) * len(self.slots) + i
        return place.batch(ref, ref, self.send.at[at], self.recv.at[at], to)

    def sends(self, up, d):
        bat, nb = self.place.bat, self.place.nb
        return (bat - d >= 0) & (bat + 1 < nb) if up else (bat + d < nb) & (bat >= 1)

    def start(self, d, parts):
        for up in (True, False):

            @pl.when(self.sends(up, d))
            def _(up=up):
                for i in parts:
                    self.copy(up, d, i).start()

    def came(self, up, d):
        return self.place.bat - d >= 0 if up else self.place.bat + d < self.place.nb

    def relay(self, d, parts, then=None):
        bat, nb = self.place.bat, self.place.nb
        for up in (True, False):

            @pl.when(self.came(up, d))
            def _(up=up):
                for i in parts:
                    block = bat - d if up else bat + d
                    ref = self.slots[i](block)
                    at = (int(up) * nb + d - 1) * len(self.slots) + i
                    self.place.batch(ref, ref, self.send.at[at], self.recv.at[at], bat).wait_recv()
                    if d < nb - 1:

                        @pl.when(self.sends(up, d))
                        def _():
                            self.copy(up, d, i).start()

                    if then:
                        then(block, up, i)

    def finish(self, parts):
        for d in range(self.place.nb - 1):
            for up in (True, False):

                @pl.when(self.sends(up, d))
                def _(up=up, d=d):
                    for i in parts:
                        self.copy(up, d, i).wait_send()


class LineSum:
    def __init__(self, place, parts, bufs, sems):
        self.place, self.parts = place, parts
        self.bufs = [bufs[4 * i : 4 * i + 4] for i in range(len(parts))]
        self.send, self.recv = sems

    @staticmethod
    def sems(nb, parts):
        return [DMA((2 * nb * parts,)), DMA((2 * nb * parts,))]

    @staticmethod
    def scratch(nb, shapes):
        slots = (nb - 1, nb - 2, nb - 1, nb - 2)
        return [pltpu.VMEM((n,) + shape, BF) for shape in shapes for n in slots]

    def copy(self, up, d, i, first):
        place = self.place
        land, acc = self.bufs[i][:2] if up else self.bufs[i][2:]
        to = place.bat + 1 if up else place.bat - 1
        dest = place.bat + d if up else place.bat - d
        src = self.parts[i](dest) if first else acc.at[d - 1]
        at = (int(up) * place.nb + d) * len(self.parts) + i
        return place.batch(src, land.at[d - 1], self.send.at[at], self.recv.at[at], to)

    def arrived(self, up, d, i):
        place = self.place
        land = self.bufs[i][0 if up else 2]
        at = (int(up) * place.nb + d + 1) * len(self.parts) + i
        place.batch(land.at[d], land.at[d], self.send.at[at], self.recv.at[at], place.bat).wait_recv()
        return land[d].astype(F32)

    def edge(self, up):
        return self.place.bat == 0 if up else self.place.bat == self.place.nb - 1

    def inside(self, up, d):
        return self.place.bat + d < self.place.nb if up else self.place.bat - d >= 0

    def start(self):
        for d in reversed(range(1, self.place.nb)):
            for up in (True, False):

                @pl.when(self.edge(up))
                def _(up=up, d=d):
                    for i in range(len(self.parts)):
                        self.copy(up, d, i, True).start()

    def stage(self, d):
        for up in (True, False):

            @pl.when(self.inside(up, d) & jnp.logical_not(self.edge(up)))
            def _(up=up):
                for i in range(len(self.parts)):
                    dest = self.place.bat + d if up else self.place.bat - d
                    acc = self.bufs[i][1 if up else 3]
                    acc[d - 1] = (self.parts[i](dest)[...].astype(F32) + self.arrived(up, d, i)).astype(BF)
                    self.copy(up, d, i, False).start()

    def total(self, outs):
        for i, out in enumerate(outs):
            out[...] = self.parts[i](self.place.bat)[...].astype(out.dtype)
            for up in (True, False):

                @pl.when(jnp.logical_not(self.edge(up)))
                def _(up=up):
                    out[...] = (out[...].astype(F32) + self.arrived(up, 0, i)).astype(out.dtype)

    def finish(self):
        for d in range(1, self.place.nb):
            for up in (True, False):

                @pl.when(self.inside(up, d) & self.edge(up))
                def _(up=up, d=d):
                    for i in range(len(self.parts)):
                        self.copy(up, d, i, True).wait_send()

                @pl.when(self.inside(up, d) & jnp.logical_not(self.edge(up)))
                def _(up=up, d=d):
                    for i in range(len(self.parts)):
                        self.copy(up, d, i, False).wait_send()


class Exchange:
    def __init__(self, place, pieces, slots, sems):
        self.place, self.pieces, self.slots = place, pieces, slots
        self.send, self.recv = sems

    @staticmethod
    def sems(ns, parts):
        return [DMA((ns * parts,)), DMA((ns * parts,))]

    def copy(self, t, i):
        place = self.place
        to = lax.rem(place.me + t, place.ns)
        at = t * len(self.pieces) + i
        src, dst = self.pieces[i](to), self.slots[i](place.me, to)
        if t == 0:
            return pltpu.make_async_copy(src, dst, self.recv.at[at])
        return place.seq(src, dst, self.send.at[at], self.recv.at[at], to)

    def start(self):
        for t in range(self.place.ns):
            for i in range(len(self.pieces)):
                self.copy(t, i).start()

    def arrive(self):
        place = self.place
        for t in range(place.ns):
            for i in range(len(self.pieces)):
                if t == 0:
                    self.copy(0, i).wait()
                    continue
                at = t * len(self.pieces) + i
                spot = self.slots[i](lax.rem(place.me + place.ns - t, place.ns), place.me)
                place.seq(spot, spot, self.send.at[at], self.recv.at[at], place.sib).wait_recv()

    def finish(self):
        for t in range(1, self.place.ns):
            for i in range(len(self.pieces)):
                self.copy(t, i).wait_send()


def take(refs, counts):
    out, at = [], 0
    for n in counts:
        out.append(refs[at : at + n])
        at += n
    return out


def comm_call(body, out_shape, scratch, cid, *args):
    return pl.pallas_call(
        body,
        out_shape=out_shape,
        in_specs=[VMEM] * len(args),
        out_specs=[VMEM] * len(out_shape),
        scratch_shapes=scratch,
        compiler_params=pltpu.CompilerParams(
            collective_id=cid, has_side_effects=True, vmem_limit_bytes=60 << 20
        ),
    )(*args)


def sds(shape, dtype):
    return jax.ShapeDtypeStruct(tuple(shape), dtype)


def half_of(v, h):
    lane = lax.broadcasted_iota(jnp.int32, v.shape, 1)
    return jnp.where(lane // HD == h, v, jnp.zeros_like(v))


def turn(v, cosine, sine):
    lane = lax.broadcasted_iota(jnp.int32, v.shape, 1)
    width, half = v.shape[1], ROPE // 2
    swapped = jnp.where((lane // half) % 2 == 0, pltpu.roll(v, width - half, 1), pltpu.roll(v, half, 1))
    return v * cosine + swapped * sine


def blocks(count, body):
    def step(i, carry):
        body(aligned(i * ROWS, ROWS))
        return carry

    lax.fori_loop(0, count, step, 0)


def normalize(r, x, gain, a):
    a[r, :] = rms(x[r, :].astype(F32), gain)[1].astype(BF)


def project(r, a, wcat, ukey, cosine, sine, q, qr, kr, c, ql):
    qkv = mm(a[r, :], wcat)
    co, si = cosine[r, :], sine[r, :]
    qt = qkv[:, :128].astype(BF)
    q[r, :] = qt
    qr[r, :] = turn(qkv[:, 128:256], co, si).astype(BF)
    kr[r, :] = turn(qkv[:, 256:384], co, si).astype(BF)
    c[r, :] = qkv[:, 384:].astype(BF)
    for h in range(2):
        ql[r, h * LAT : (h + 1) * LAT] = mm(half_of(qt, h), ukey).astype(BF)


def scores(i, h, q_lat, q_rope, c, kr):
    n = (i + 1) * ROWS
    s = (mm_nt(q_lat, c[:n, :]) + mm_nt(half_of(q_rope, h), kr[:n, :])) * SCALE
    row = lax.broadcasted_iota(jnp.int32, (ROWS, ROWS), 0)
    col = lax.broadcasted_iota(jnp.int32, (ROWS, ROWS), 1)
    own = jnp.where(col <= row, s[:, n - ROWS :], NEG_FILL)
    return own if i == 0 else jnp.concatenate([s[:, : n - ROWS], own], 1)


def attend(i, q_lat, q_rope, c, kr, uval, wout, ol, lse, o, part):
    n, r = (i + 1) * ROWS, pl.ds(i * ROWS, ROWS)
    outs = []
    for h in range(2):
        w = slice(h * LAT, (h + 1) * LAT)
        s = scores(i, h, q_lat[r, w], q_rope[r, :], c, kr)
        top = jnp.max(s, -1, keepdims=True)
        e = jnp.exp(s - top)
        total = jnp.sum(e, -1, keepdims=True)
        v = mm(e.astype(BF), c[:n, :]) / total
        ol[r, w] = v
        lse[h, r, :] = jnp.broadcast_to(top + jnp.log(total), (ROWS, 128))
        outs.append(half_of(mm_nt(v.astype(BF), uval), h))
    ot = (outs[0] + outs[1]).astype(BF)
    o[r, :] = ot
    part[r, :] = mm(ot, wout).astype(BF)


def attend_back(i, first, q_lat, q_rope, c, kr, uval, ukey, wout, ol, lse, o, q, dat, cosine, sine, dc, dk, sums, gcat):
    n, r = (i + 1) * ROWS, pl.ds(i * ROWS, ROWS)
    d = dat[r, :]
    do = mm_nt(d, wout).astype(BF)
    out_grad = mm_tn(o[r, :], d)
    qt = q[r, :]
    dq, dqr, uk, uv = 0.0, 0.0, 0.0, 0.0
    for h in range(2):
        w = slice(h * LAT, (h + 1) * LAT)
        doh = half_of(do, h)
        out = ol[r, w]
        uv = uv + mm_tn(doh, out.astype(BF))
        dol = mm(doh, uval).astype(BF)
        delta = jnp.sum(dol.astype(F32) * out, -1, keepdims=True)
        lat = q_lat[r, w]
        p = jnp.exp(scores(i, h, lat, q_rope[r, :], c, kr) - lse[h, r, :][:, :1])
        ds = (p * ((mm_nt(dol, c[:n, :]) - delta) * SCALE)).astype(BF)
        dql = mm(ds, c[:n, :]).astype(BF)
        dqr = dqr + half_of(mm(ds, kr[:n, :]), h)
        dc_new = mm_tn(jnp.concatenate([p.astype(BF), ds], 0), jnp.concatenate([dol, lat], 0))
        dk_new = mm_tn(ds, half_of(q_rope[r, :], h))
        if first and h == 0:
            dc[:n, :] = dc_new
            dk[:n, :] = dk_new
        else:
            dc[:n, :] += dc_new
            dk[:n, :] += dk_new
        uk = uk + mm_tn(half_of(qt, h), dql)
        dq = dq + half_of(mm_nt(dql, ukey), h)
    for ref, value in zip(sums, (uk, uv, out_grad)):
        if first:
            ref[...] = value
        else:
            ref[...] += value
    co, si = cosine[r, :], -sine[r, :]
    gcat[r, :128] = dq.astype(BF)
    gcat[r, 128:256] = turn(dqr, co, si).astype(BF)
    gcat[r, 256:384] = turn(dk[r, :], co, si).astype(BF)
    gcat[r, 384:] = dc[r, :].astype(BF)


def seq_gather(v):
    return lax.all_gather(v, "seq", axis=0, tiled=True)


def seq_sum(v):
    return lax.psum_scatter(v.astype(BF), "seq", scatter_dimension=0, tiled=True).astype(F32)


def batch_gather(v):
    return lax.all_gather(v, "batch", axis=0, tiled=True)


def batch_sum(v):
    return lax.psum_scatter(v.astype(BF), "batch", scatter_dimension=0, tiled=True).astype(F32)


def plain(
    tokens,
    out_grad,
    group_id,
    group_weight,
    gain_attn,
    w_query,
    w_qrope,
    w_latent,
    w_krope,
    w_ukey,
    w_uval,
    w_out,
    gain_ffn,
    w_gate,
    w_up,
    w_down,
):
    ns, nb = lax.axis_size("seq"), lax.axis_size("batch")
    seq_count, rows, width = tokens.shape
    shard = w_query.shape[0]
    length = rows * ns
    hl = H // ns
    fl = FF // ns
    qw, rw = hl * HD, hl * ROPE
    scaling = (HD + ROPE) ** (-0.5)

    def columns(w, blocks):
        return w.astype(BF).reshape(shard, blocks, -1).transpose(1, 0, 2)

    lat_cols = jnp.repeat(columns(w_latent, GROUPS), ns // GROUPS, axis=0)
    kr_cols = jnp.broadcast_to(w_krope.astype(BF)[None], (ns, shard, ROPE))
    send = jnp.concatenate(
        [columns(w_query, ns), columns(w_qrope, ns), lat_cols, kr_cols, columns(w_gate, ns), columns(w_up, ns)], -1
    )
    got = lax.all_to_all(send, "seq", 0, 0)
    wide = send.shape[-1]
    full = lax.all_gather(got, "batch", axis=1).reshape(width, wide)
    attn_w = qw + rw + LAT + ROPE
    wcat, wgu = full[:, :attn_w], full[:, attn_w:]
    ukey = batch_gather(w_ukey.astype(BF))
    uval = batch_gather(w_uval.astype(BF))
    wout = batch_gather(w_out.astype(BF))
    wdown = batch_gather(w_down.astype(BF))
    gains = lax.all_gather(
        jnp.stack([gain_attn, gain_ffn]).astype(BF), ("seq", "batch"), axis=1, tiled=True
    ).astype(F32)
    gain_a, gain_f = gains[0], gains[1]

    x = tokens.reshape(rows, width)
    domains = jnp.arange(group_weight.shape[0])
    seq_weight = jnp.sum(jnp.where(group_id[:, None] == domains[None, :], group_weight[None, :], 0.0), -1)
    gy = (out_grad.astype(F32) * seq_weight[:, None, None]).reshape(rows, width)
    dy_all = seq_gather(gy.astype(BF))
    x_all = seq_gather(x)
    x32 = x.astype(F32)

    position = jnp.arange(length).astype(F32)
    freq = ROTARY_BASE ** (-jnp.arange(ROPE // 2).astype(F32) * 2.0 / ROPE)
    angles = position[:, None] * freq
    cosine, sine = jnp.cos(angles), jnp.sin(angles)

    _, normed = rms(x_all.astype(F32), gain_a)
    a_all = normed.astype(BF)
    qkv = mm(a_all, wcat)
    q = qkv[:, :qw].astype(BF)
    qr = rotate(qkv[:, qw : qw + rw].reshape(length, hl, ROPE), cosine[:, None], sine[:, None]).astype(BF)
    c = qkv[:, qw + rw : qw + rw + LAT].astype(BF)
    kr = rotate(qkv[:, qw + rw + LAT :], cosine, sine).astype(BF)
    causal = jnp.arange(length)[None, :] <= jnp.arange(length)[:, None]

    keep = []
    outs = []
    for h in range(hl):
        uh = ukey[h * HD : (h + 1) * HD]
        vh = uval[h * HD : (h + 1) * HD]
        ql = mm(q[:, h * HD : (h + 1) * HD], uh).astype(BF)
        sc = (mm_nt(ql, c) + mm_nt(qr[:, h], kr)) * scaling
        sc = jnp.where(causal, sc, NEG_FILL)
        top = jnp.max(sc, -1, keepdims=True)
        e = jnp.exp(sc - top)
        total = jnp.sum(e, -1, keepdims=True)
        ol = mm(e.astype(BF), c) / total
        olb = ol.astype(BF)
        outs.append(mm_nt(olb, vh).astype(BF))
        keep.append((ql, ol, olb, top + jnp.log(total)))
    o = jnp.concatenate(outs, -1)
    hres = x32 + seq_sum(mm(o, wout))
    inv_f, normed_f = rms(hres, gain_f)
    b_all = seq_gather(normed_f.astype(BF))
    gu = mm(b_all, wgu)
    gate, up = gu[:, :fl], gu[:, fl:]
    sig = jax.nn.sigmoid(gate)
    act = gate * sig
    hid = (act * up).astype(BF)
    y = seq_sum(mm(hid, wdown))
    result = (hres + y).astype(BF).reshape(seq_count, rows, width)

    dhid = mm_nt(dy_all, wdown)
    dgate = (dhid * up * sig * (1.0 + gate * (1.0 - sig))).astype(BF)
    dup = (dhid * act).astype(BF)
    dgu = jnp.concatenate([dgate, dup], -1)
    db = seq_sum(mm_nt(dgu, wgu))
    g_down = batch_sum(mm_tn(hid, dy_all))
    g_gu = mm_tn(b_all, dgu)
    back_f, gg_f = rms_grad(hres, inv_f, gain_f, db)
    dres = gy + back_f
    dat_all = seq_gather(dres.astype(BF))
    g_out = mm_tn(o, dat_all)
    do = mm_nt(dat_all, wout).astype(BF)

    dqs, dqps, g_uk, g_uv = [], [], [], []
    dc = jnp.zeros((length, LAT), F32)
    dkr = jnp.zeros((length, ROPE), F32)
    for h in range(hl):
        ql, ol, olb, lse = keep[h]
        uh = ukey[h * HD : (h + 1) * HD]
        vh = uval[h * HD : (h + 1) * HD]
        doh = do[:, h * HD : (h + 1) * HD]
        g_uv.append(mm_tn(doh, olb))
        dol = mm(doh, vh).astype(BF)
        delta = jnp.sum(dol.astype(F32) * ol, -1, keepdims=True)
        sc = (mm_nt(ql, c) + mm_nt(qr[:, h], kr)) * scaling
        p = jnp.exp(jnp.where(causal, sc, NEG_FILL) - lse)
        ds = (p * (mm_nt(dol, c) - delta)).astype(BF)
        dql = (scaling * mm(ds, c)).astype(BF)
        dqps.append(rotate(scaling * mm(ds, kr), cosine, -sine).astype(BF))
        dkr = dkr + scaling * mm_tn(ds, qr[:, h])
        dc = dc + mm_tn(p.astype(BF), dol) + scaling * mm_tn(ds, ql)
        g_uk.append(mm_tn(q[:, h * HD : (h + 1) * HD], dql))
        dqs.append(mm_nt(dql, uh).astype(BF))
    dkp = rotate(dkr, cosine, -sine).astype(BF)
    gcat = jnp.concatenate(dqs + dqps + [dc.astype(BF), dkp], -1)
    da = seq_sum(mm_nt(gcat, wcat))
    g_cat = mm_tn(a_all, gcat)
    inv_a, _ = rms(x32, gain_a)
    back_a, gg_a = rms_grad(x32, inv_a, gain_a, da)
    input_grad = (dres + back_a).reshape(seq_count, rows, width)

    def wide_sum(g):
        cols = g.shape[-1]
        part = lax.psum_scatter(
            g.astype(BF).reshape(ns, nb, shard, cols), "batch", scatter_dimension=1, tiled=True
        ).reshape(ns, shard, cols)
        return lax.all_to_all(part, "seq", 0, 0)

    def spread(v):
        return v.transpose(1, 0, 2).reshape(shard, -1)

    r_gu = wide_sum(g_gu)
    r_cat = wide_sum(g_cat).astype(F32)
    p_query = spread(r_cat[:, :, :qw])
    p_qrope = spread(r_cat[:, :, qw : qw + rw])
    p_latent = spread(
        r_cat[:, :, qw + rw : qw + rw + LAT].reshape(GROUPS, ns // GROUPS, shard, LAT).sum(1)
    )
    p_krope = r_cat[:, :, qw + rw + LAT :].sum(0)
    p_gate = spread(r_gu[:, :, :fl]).astype(F32)
    p_up = spread(r_gu[:, :, fl:]).astype(F32)
    g_head = batch_sum(jnp.concatenate([jnp.concatenate(g_uk, 0), jnp.concatenate(g_uv, 0), g_out], -1))
    gg = lax.psum_scatter(jnp.concatenate([gg_a, gg_f]), ("seq", "batch"), scatter_dimension=1, tiled=True)
    return (
        result,
        input_grad,
        gg[0],
        p_query,
        p_qrope,
        p_latent,
        p_krope,
        g_head[:, :LAT],
        g_head[:, LAT : 2 * LAT],
        g_head[:, 2 * LAT :],
        gg[1],
        p_gate,
        p_up,
        g_down,
    )


class Total:
    def __init__(self, place, own, by_seq, by_batch, sems):
        self.place, self.own, self.by_seq, self.by_batch = place, own, by_seq, by_batch
        self.over = Exchange(place, [lambda to: own], [lambda frm, to: by_seq.at[frm]], sems[:2])
        self.send, self.recv = sems[2:]

    @staticmethod
    def scratch(ns, nb, shape):
        return [pltpu.VMEM(shape, F32), pltpu.VMEM((ns,) + shape, F32), pltpu.VMEM((nb,) + shape, F32)]

    @staticmethod
    def sems(ns, nb):
        return Exchange.sems(ns, 1) + [DMA((nb,)), DMA((nb,))]

    def start(self):
        self.over.start()

    def copy(self, t):
        place = self.place
        to = lax.rem(place.bat + t, place.nb)
        return place.batch(self.own, self.by_batch.at[place.bat], self.send.at[t], self.recv.at[t], to)

    def middle(self):
        self.over.arrive()
        self.over.finish()
        self.own[...] = jnp.sum(self.by_seq[...], 0)
        for t in range(1, self.place.nb):
            self.copy(t).start()
        self.by_batch[self.place.bat] = self.own[...]

    def result(self):
        place = self.place
        for t in range(1, place.nb):
            spot = self.by_batch.at[lax.rem(place.bat + place.nb - t, place.nb)]
            place.batch(spot, spot, self.send.at[t], self.recv.at[t], place.bat).wait_recv()
        return jnp.sum(self.by_batch[...], 0)

    def finish(self):
        for t in range(1, self.place.nb):
            self.copy(t).wait_send()


def rotations(length, freq, cosine, sine):
    def fill(r):
        spot = lax.broadcasted_iota(jnp.int32, (ROWS, 128), 0) + r.start
        angle = spot.astype(F32) * freq[...]
        lane = lax.broadcasted_iota(jnp.int32, (ROWS, 128), 1)
        cosine[r, :] = jnp.cos(angle)
        turned = jnp.sin(angle)
        sine[r, :] = jnp.where((lane // (ROPE // 2)) % 2 == 0, -turned, turned)

    blocks(length // ROWS, fill)


def forward(ns, nb, x, out_grad, group, weights, gains, freq, params, chunks=4):
    rows, width = x.shape
    length = ns * rows
    shard = params[0].shape[0]
    qk = 2 * (HD + ROPE) + 2 * ROPE
    full = qk + LAT
    fl = params[8].shape[1] // ns
    down = params[9]
    head_w = 2 * LAT + width

    def body(x, og, gid, gws, gin, fr, wq, wqr, wl, wkr, wuk, wuv, wo, wg, wu, wd, *rest):
        outs, rest = rest[:20], rest[20:]
        dy_all, a_all, wc, hrow, fcol, drow, q, qr, kr, c, ql, ol, lse, o, hres, b_all, gout, gy, co, si = outs
        x_all, part, own, dy, wa, wf = rest[:6]
        bufs, tot, gx, gd, ea, ef, zl, zf, sib, rs, gs, ts, local = take(
            rest[6:], (3, 3, 4, 4, 2, 2, 2, 2, 2, 4, 4, 4, 1)
        )
        place = Place(ns, nb)
        local = local[0]
        mine = aligned(place.me * rows, rows)
        gain = Total(place, *tot, ts)
        lane = lax.broadcasted_iota(jnp.int32, (2, width), 1)
        mask = lane // shard == place.me * nb + place.bat
        gain.own[...] = jnp.where(mask, gin[...].astype(BF).astype(F32), 0.0)
        for s in range(ns):
            half_at = (s // (ns // GROUPS)) * LAT + (s % 2) * HALF
            wa[s, :, : 2 * HD] = wq[:, s * 2 * HD : (s + 1) * 2 * HD].astype(BF)
            wa[s, :, 2 * HD : 2 * (HD + ROPE)] = wqr[:, s * 2 * ROPE : (s + 1) * 2 * ROPE].astype(BF)
            wa[s, :, qk - 2 * ROPE : qk] = jnp.concatenate([wkr[...], wkr[...]], 1).astype(BF)
            wa[s, :, qk:] = wl[:, half_at : half_at + HALF].astype(BF)
        hrow[place.bat, :, :LAT] = wuk[...].astype(BF)
        hrow[place.bat, :, LAT : 2 * LAT] = wuv[...].astype(BF)
        hrow[place.bat, :, 2 * LAT :] = wo[...].astype(BF)
        copies = [pltpu.make_async_copy(x, x_all.at[mine], local.at[0])]
        copies[0].start()
        place.barrier(True, True)

        def half(core):
            return pl.ds(pl.multiple_of(qk + HALF * core, HALF), HALF)

        cols = Exchange(
            place,
            [lambda to: wa.at[to, :, pl.ds(0, qk)], lambda to: wa.at[to, :, pl.ds(qk, HALF)]],
            [
                lambda frm, to: wc.at[frm, place.bat, :, pl.ds(0, qk)],
                lambda frm, to: wc.at[frm, place.bat, :, half(lax.rem(to, 2))],
            ],
            ea,
        )
        ffn = Exchange(place, [lambda to: wf.at[to]], [lambda frm, to: fcol.at[frm, place.bat]], ef)
        along = Line(
            place,
            [
                lambda b: hrow.at[b],
                lambda b: wc.at[:, b, :, pl.ds(0, qk)],
                lambda b: wc.at[:, b, :, half(place.core)],
            ],
            zl,
        )
        later = Line(place, [lambda b: fcol.at[:, b], lambda b: drow.at[b]], zf)

        def to_sibling(b, i):
            ref = wc.at[:, b, :, half(place.core)]
            return place.seq(ref, ref, sib[0].at[i], sib[1].at[i], place.sib)

        def from_sibling(b, i):
            ref = wc.at[:, b, :, half(1 - place.core)]
            place.seq(ref, ref, sib[0].at[i], sib[1].at[i], place.sib).wait_recv()

        def pass_on(d):
            along.relay(d, [0, 1])
            along.relay(d, [2], lambda b, up, i: to_sibling(b, d if up else nb - 1 + d).start())

        xs, ds = Gather(place, x, x_all, chunks, gx), Gather(place, dy, dy_all, chunks, gd)
        cols.start()
        along.start(0, [0])
        gain.start()
        xs.start()
        weight = jnp.sum(jnp.where(lax.broadcasted_iota(jnp.int32, gws.shape, 1) == gid[...], gws[...], 0.0), -1)
        gy[...] = og[...].astype(F32) * weight[:, None]
        dy[...] = gy[...].astype(BF)
        dy_all[mine, :] = dy[...]
        for s in range(ns):
            wf[s, :, :fl] = wg[:, s * fl : (s + 1) * fl].astype(BF)
            wf[s, :, fl:] = wu[:, s * fl : (s + 1) * fl].astype(BF)
        drow[place.bat] = wd[...].astype(BF)
        cols.arrive()
        along.start(0, [1, 2])
        to_sibling(place.bat, 0).start()
        gain.middle()
        xs.relay()
        ffn.start()
        ds.start()
        pass_on(1)
        gout[...] = gain.result()
        copies[0].wait()
        xs.finish()
        blocks(length // ROWS, lambda r: normalize(r, x_all, gout[pl.ds(0, 1), :], a_all))
        pass_on(2)
        rotations(length, fr, co, si)
        ffn.arrive()
        later.start(0, [0, 1])
        for d in range(3, nb):
            pass_on(d)
        from_sibling(place.bat, 0)
        for d in range(1, nb):
            for up in (True, False):

                @pl.when(along.came(up, d))
                def _(up=up, d=d):
                    from_sibling(place.bat - d if up else place.bat + d, d if up else nb - 1 + d)

        ds.relay()
        wcat = wc[...].reshape(width, full)
        heads = hrow[...].reshape(nb * shard, head_w)
        ukey, uval, wout = heads[:, :LAT], heads[:, LAT : 2 * LAT], heads[:, 2 * LAT :]
        blocks(length // ROWS, lambda r: project(r, a_all, wcat, ukey, co, si, q, qr, kr, c, ql))
        for i in range(length // ROWS):
            attend(i, ql, qr, c, kr, uval, wout, ol, lse, o, part)
        sums = Scatter(place, part, bufs, rs)
        sums.start()
        later.relay(1, [0, 1])
        value = x[...].astype(F32) + sums.total()
        hres[...] = value
        own[...] = rms(value, gout[pl.ds(1, 1), :])[1].astype(BF)
        spread = Gather(place, own, b_all, chunks, gs)
        spread.start()
        last_copy = pltpu.make_async_copy(own, b_all.at[mine], local.at[1])
        last_copy.start()
        later.relay(2, [0, 1])
        spread.relay()
        for d in range(3, nb):
            later.relay(d, [0, 1])
        spread.finish()
        sums.finish()
        ds.finish()
        cols.finish()
        ffn.finish()
        along.finish([0, 1, 2])
        later.finish([0, 1])
        gain.finish()
        to_sibling(place.bat, 0).wait_send()
        for d in range(1, nb):
            for up in (True, False):

                @pl.when(along.came(up, d))
                def _(up=up, d=d):
                    to_sibling(place.bat - d if up else place.bat + d, d if up else nb - 1 + d).wait_send()

        last_copy.wait()

    scratch = (
        [pltpu.VMEM((length, width), BF)] * 2
        + [pltpu.VMEM((rows, width), BF)] * 2
        + [pltpu.VMEM((ns, shard, qk + HALF), BF), pltpu.VMEM((ns, shard, 2 * fl), BF)]
        + Scatter.bufs(ns, rows, width)
        + Total.scratch(ns, nb, (2, width))
        + Gather.sems(ns, chunks)
        + Gather.sems(ns, chunks)
        + Exchange.sems(ns, 2)
        + Exchange.sems(ns, 1)
        + Line.sems(nb, 3)
        + Line.sems(nb, 2)
        + [DMA((2 * nb,)), DMA((2 * nb,))]
        + Scatter.sems(ns)
        + Gather.sems(ns, chunks)
        + Total.sems(ns, nb)
        + [DMA((2,))]
    )
    return comm_call(
        body,
        [
            sds((length, width), BF),
            sds((length, width), BF),
            sds((ns, nb, shard, full), BF),
            sds((nb, shard, head_w), BF),
            sds((ns, nb, shard, 2 * fl), BF),
            sds((nb,) + down.shape, BF),
            sds((length, 128), BF),
            sds((length, 128), BF),
            sds((length, 128), BF),
            sds((length, LAT), BF),
            sds((length, 2 * LAT), BF),
            sds((length, 2 * LAT), F32),
            sds((2, length, 128), F32),
            sds((length, 128), BF),
            sds((rows, width), F32),
            sds((length, width), BF),
            sds((2, width), F32),
            sds((rows, width), F32),
            sds((length, 128), F32),
            sds((length, 128), F32),
        ],
        scratch,
        1,
        x,
        out_grad,
        group,
        weights,
        gains,
        freq,
        *params,
    )


def backward(ns, nb, part_db, part_y, gy, hres, x, gains, g_wide, g_down, saved, chunks=4):
    rows, width = x.shape
    length = ns * rows
    shard = g_wide.shape[2]
    full = saved[1].shape[-1]
    head_w = saved[2].shape[-1]
    block = (ns, shard, full)

    def body(pdb, py, gy, hres, x, gains, gw, gd, a_all, wc, hrow, q, qr, kr, c, ql, ol, lse, o, co, si, *rest):
        dx, y, gg, c_out, r_out, w_out, d_out = rest[:7]
        own, dres, dat_all, pda, dc, dk, uk, uv, og, gcat, gc, gr, c_sum, w_sum = rest[7:21]
        bd, by, ba, zfb, zab, tot, rd, ry, ra, gs, zf, za, ec, ew, ts, local = take(
            rest[21:], (3, 3, 3, 8, 8, 3, 4, 4, 4, 4, 2, 2, 2, 2, 4, 1)
        )
        place = Place(ns, nb)
        gain_a, gain_f = gains[pl.ds(0, 1), :], gains[pl.ds(1, 1), :]
        place.barrier(True, True)
        sums = Scatter(place, pdb, bd, rd)
        outs = Scatter(place, py, by, ry)
        later = LineSum(place, [lambda b: gw.at[:, b], lambda b: gd.at[b]], zfb, zf)
        sums.start()
        later.start()
        db = sums.total()
        value = hres[...]
        back, gg_f = rms_grad(value, rms(value, gain_f)[0], gain_f, db)
        value = gy[...] + back
        dres[...] = value
        own[...] = value.astype(BF)
        spread = Gather(place, own, dat_all, chunks, gs)
        spread.start()
        copy = pltpu.make_async_copy(own, dat_all.at[aligned(place.me * rows, rows)], local[0].at[0])
        copy.start()
        for d in reversed(range(2, nb - 1)):
            later.stage(d)
        spread.relay()
        outs.start()
        copy.wait()
        spread.finish()
        wcat = wc[...].reshape(width, full)
        heads = hrow[...].reshape(nb * shard, head_w)
        ukey, uval, wout = heads[:, :LAT], heads[:, LAT : 2 * LAT], heads[:, 2 * LAT :]
        wide = Exchange(place, [lambda to: w_sum.at[to]], [lambda frm, to: w_out.at[frm]], ew)
        count = length // ROWS
        todo = list(reversed(range(1, place.nc)))
        for i in reversed(range(count)):
            attend_back(
                i, i == count - 1, ql, qr, c, kr, uval, ukey, wout, ol, lse, o, q, dat_all, co, si, dc, dk, (uk, uv, og), gcat
            )
            if i == count - 1:
                later.stage(1)
            if todo:
                outs.step(todo.pop(0))
        for mask in todo:
            outs.step(mask)
        for j in range(ns):
            g = mm_tn(a_all[:, j * nb * shard : (j + 1) * nb * shard], gcat[...])
            gc[j] = g.astype(BF).reshape(nb, shard, full)
        heads_grad = jnp.concatenate([uk[...], uv[...], og[...]], 1)
        gr[...] = heads_grad.astype(BF).reshape(nb, shard, head_w)
        along = LineSum(place, [lambda b: gc.at[:, b], lambda b: gr.at[b]], zab, za)
        along.start()

        def da_block(r):
            pda[r, :] = mm_nt(gcat[r, :], wcat).astype(BF)

        blocks(count, da_block)
        ins = Scatter(place, pda, ba, ra)
        ins.start()
        later.total([w_sum, d_out])
        wide.start()
        y[...] = (hres[...] + outs.step(0)).astype(BF)
        for d in reversed(range(2, nb - 1)):
            along.stage(d)
        da = ins.total()
        value = x[...].astype(F32)
        back, gg_a = rms_grad(value, rms(value, gain_a)[0], gain_a, da)
        dx[...] = dres[...] + back
        gain = Total(place, *tot, ts)
        gain.own[pl.ds(0, 1), :] = gg_a
        gain.own[pl.ds(1, 1), :] = gg_f
        gain.start()
        along.stage(1)
        gain.middle()
        along.total([c_sum, r_out])
        cols = Exchange(place, [lambda to: c_sum.at[to]], [lambda frm, to: c_out.at[frm]], ec)
        cols.start()
        gg[...] = gain.result()
        wide.arrive()
        cols.arrive()
        for job in (gain, sums, outs, ins, later, along, wide, cols):
            job.finish()

    scratch = (
        [
            pltpu.VMEM((rows, width), BF),
            pltpu.VMEM((rows, width), F32),
            pltpu.VMEM((length, width), BF),
            pltpu.VMEM((length, width), BF),
            pltpu.VMEM((length, LAT), F32),
            pltpu.VMEM((length, 128), F32),
            pltpu.VMEM((128, LAT), F32),
            pltpu.VMEM((128, LAT), F32),
            pltpu.VMEM((128, width), F32),
            pltpu.VMEM((length, full), BF),
            pltpu.VMEM((ns, nb, shard, full), BF),
            pltpu.VMEM((nb, shard, head_w), BF),
            pltpu.VMEM(block, BF),
            pltpu.VMEM((ns,) + g_wide.shape[2:], BF),
        ]
        + Scatter.bufs(ns, rows, width) * 3
        + LineSum.scratch(nb, [(ns,) + g_wide.shape[2:], g_down.shape[1:]])
        + LineSum.scratch(nb, [block, (shard, head_w)])
        + Total.scratch(ns, nb, (2, width))
        + Scatter.sems(ns) * 3
        + Gather.sems(ns, chunks)
        + LineSum.sems(nb, 2)
        + LineSum.sems(nb, 2)
        + Exchange.sems(ns, 1)
        + Exchange.sems(ns, 1)
        + Total.sems(ns, nb)
        + [DMA((1,))]
    )
    return comm_call(
        body,
        [
            sds((rows, width), F32),
            sds((rows, width), BF),
            sds((2, width), F32),
            sds(block, BF),
            sds((shard, head_w), F32),
            sds((ns,) + g_wide.shape[2:], BF),
            sds(g_down.shape[1:], F32),
        ],
        scratch,
        2,
        part_db,
        part_y,
        gy,
        hres,
        x,
        gains,
        g_wide,
        g_down,
        *saved,
    )


def deliver(ns, cols, wide, heads, down, dx, y):
    shard, width = cols.shape[1], dx.shape[1]
    fl = wide.shape[2] // 2
    qk = 2 * (HD + ROPE)

    def body(cols, wide, heads, down, dx, y, y_out, dx_out, gq, gqr, gl, gk, guk, guv, go, gg, gu, gd):
        y_out[...] = y[...]
        dx_out[...] = dx[...]
        kr = jnp.zeros((shard, 2 * ROPE), F32)
        for s in range(ns):
            gq[:, s * 2 * HD : (s + 1) * 2 * HD] = cols[s, :, : 2 * HD].astype(F32)
            gqr[:, s * 2 * ROPE : (s + 1) * 2 * ROPE] = cols[s, :, 2 * HD : qk].astype(F32)
            kr = kr + cols[s, :, qk : qk + 2 * ROPE].astype(F32)
            gg[:, s * fl : (s + 1) * fl] = wide[s, :, :fl].astype(F32)
            gu[:, s * fl : (s + 1) * fl] = wide[s, :, fl:].astype(F32)
        gk[...] = kr[:, :ROPE] + kr[:, ROPE:]
        each = ns // GROUPS
        for g in range(GROUPS):
            total = cols[g * each, :, qk + 2 * ROPE :].astype(F32)
            for s in range(g * each + 1, (g + 1) * each):
                total = total + cols[s, :, qk + 2 * ROPE :].astype(F32)
            gl[:, g * LAT : (g + 1) * LAT] = total
        guk[...] = heads[:, :LAT]
        guv[...] = heads[:, LAT : 2 * LAT]
        go[...] = heads[:, 2 * LAT :]
        gd[...] = down[...]

    shapes = [
        sds(y.shape, BF),
        sds(dx.shape, F32),
        sds((shard, ns * 2 * HD), F32),
        sds((shard, ns * 2 * ROPE), F32),
        sds((shard, GROUPS * LAT), F32),
        sds((shard, ROPE), F32),
        sds((shard, LAT), F32),
        sds((shard, LAT), F32),
        sds((shard, width), F32),
        sds((shard, ns * fl), F32),
        sds((shard, ns * fl), F32),
        sds(down.shape, F32),
    ]
    return pl.pallas_call(body, out_shape=shapes, in_specs=[VMEM] * 6, out_specs=[VMEM] * len(shapes))(
        cols, wide, heads, down, dx, y
    )


def local(
    tokens,
    out_grad,
    group_id,
    group_weight,
    gain_attn,
    w_query,
    w_qrope,
    w_latent,
    w_krope,
    w_ukey,
    w_uval,
    w_out,
    gain_ffn,
    w_gate,
    w_up,
    w_down,
):
    ns, nb = lax.axis_size("seq"), lax.axis_size("batch")
    me, bat = lax.axis_index("seq"), lax.axis_index("batch")
    seq_count, rows, width = tokens.shape
    shard = w_query.shape[0]
    length = rows * ns
    fl = FF // ns

    x = tokens.reshape(rows, width)
    gains = jnp.tile(jnp.stack([gain_attn, gain_ffn]), (1, width // shard))
    steps = np.arange(ROPE // 2, dtype=np.float32) * np.float32(-2.0 / ROPE)
    freq = jnp.asarray(np.tile(np.power(np.float32(ROTARY_BASE), steps), 4)[None])
    (
        dy_all, a_all, wc, hrow, fcol, drow, q, qr, kr, c, ql, ol, lse, o, hres, b_all, gains, gy, cosine, sine
    ) = forward(
        ns,
        nb,
        x,
        out_grad.reshape(rows, width),
        group_id[:, None],
        group_weight[None, :],
        gains,
        freq,
        (w_query, w_qrope, w_latent, w_krope, w_ukey, w_uval, w_out, w_gate, w_up, w_down),
    )
    wgu = fcol.reshape(width, 2 * fl)
    wdown = drow.reshape(fl, width)
    gu = mm(b_all, wgu)
    gate, up = gu[:, :fl], gu[:, fl:]
    sig = jax.nn.sigmoid(gate)
    act = gate * sig
    hid = (act * up).astype(BF)
    part_y = mm(hid, wdown).astype(BF)
    dhid = mm_nt(dy_all, wdown)
    dgate = (dhid * up * sig * (1.0 + gate * (1.0 - sig))).astype(BF)
    dup = (dhid * act).astype(BF)
    dgu = jnp.concatenate([dgate, dup], -1)
    g_down = mm_tn(hid, dy_all).astype(BF).reshape(nb, fl // nb, width)
    g_gu = mm_tn(b_all, dgu).astype(BF).reshape(ns, nb, shard, 2 * fl)
    part_db = mm_nt(dgu, wgu).astype(BF)

    dx, y, gg, r_cat, p_head, r_gu, p_down = backward(
        ns,
        nb,
        part_db,
        part_y,
        gy,
        hres,
        x,
        gains,
        g_gu,
        g_down,
        (a_all, wc, hrow, q, qr, kr, c, ql, ol, lse, o, cosine, sine),
    )

    grads = deliver(ns, r_cat, r_gu, p_head, p_down, dx, y)
    gg = lax.dynamic_slice(gg, (0, (me * nb + bat) * shard), (2, shard))
    return (
        grads[0].reshape(seq_count, rows, width),
        grads[1].reshape(seq_count, rows, width),
        gg[0],
        *grads[2:9],
        gg[1],
        *grads[9:],
    )


def solution(mesh):
    token, row, flat = P("batch", "seq", None), P(("seq", "batch"), None), P(("seq", "batch"))
    ns, nb = mesh.shape["seq"], mesh.shape["batch"]
    fits = H == 2 * ns and (WIDTH // (ns * nb)) % 16 == 0 and nb > 2
    return jax.shard_map(
        local if fits else plain,
        mesh=mesh,
        in_specs=(token, token, P("batch"), P(), flat, row, row, row, row, row, row, row, flat, row, row, row),
        out_specs=(token, token, flat, row, row, row, row, row, row, row, flat, row, row, row),
        check_vma=False,
    )
```
